1024 devices in a mesh: fsdp: 16 (over y_lo, x), tp: 8 (over y_hi, core), rep: 8 (over z).
Axes of the slice: x: 8, y: 8 (y_hi: 4, y_lo: 2; y = y_hi * 2 + y_lo), z: 8, core: 2. Of those that a mesh axis runs over, the one named last changes fastest.
Arguments:
- tokens: bfloat16 [16384, 5120], P('fsdp', 'rep'), may hold values from -6 to 6
- ref_qkv: bfloat16 [5120, 7168], P(('rep', 'fsdp'), 'tp'), may hold values from -0.078125 to 0.078125
- ref_bias: float32 [7168], P('tp'), may hold values from -9 to 9
- segment_ids: int32 [16, 1024], P('fsdp'), may hold values from 0 to 7, never falling along the last dimension, each value on 1 to 512 neighbouring positions
- policy_key: bfloat16 [5120, 1024], P(('rep', 'fsdp'), 'tp'), may hold values from -0.078125 to 0.078125
Outputs:
- context: bfloat16 [16384, 5120], P(('fsdp', 'rep'), 'tp')
- policy_key_tp: bfloat16 [5120, 1024], P(None, 'tp')
The draws below stay inside these ranges and needn't reach their ends.
All inputs are finite; a program needn't handle non-finite values.
Results may differ from the reference program's by a relative error of at most 0.0093.
Values may be sent and summed in bfloat16 or wider, within the bound.
No kernel may reach another device: no remote copies, remote signals or barrier semaphores. Data moves between devices by JAX's collectives and lax.ppermute only.
A program may use at most 32 MiB of HBM per device.

```python
import math
import jax
import jax.numpy as jnp
import numpy as np
from jax import lax

D = 5120
QH = 40
KVH = 8
HD = 128
TOK_DEV = 1024
TOKENS = 16384
N_FSDP = 16


def draw_ref_bias(key, part):
    width = (QH + 2 * KVH) * HD
    return jnp.clip(0.5 * jax.random.normal(key, (width,), jnp.float32), -3.0, 3.0)


def steps_of(own_key, dims, cuts, least, top_value):
    def one(position, parts):
        steps = jax.random.uniform(jax.random.fold_in(jax.random.fold_in(own_key, 6), position), (parts,), jnp.float32, least / len(cuts), top_value / len(cuts))
        return jnp.repeat(jnp.exp(steps), dims[position] // parts).reshape((-1,) + (1,) * (len(dims) - position - 1))

    level = one(*cuts[0])
    for cut in cuts[1:]:
        level = level * one(*cut)
    return level


def profile(amount, total, bound, skew):
    portions = [(1 << 20) // math.isqrt(rank ** skew) + 1 for rank in range(2, amount + 1)]
    spare, counts = total - bound - (amount - 1), [1] * (amount - 1)
    while spare > 0:
        free = [i for i in range(amount - 1) if counts[i] < bound]
        mass, remaining = sum([portions[i] for i in free]), spare
        for i in free:
            extra = min(bound - counts[i], max(1, remaining * portions[i] // mass), spare)
            counts[i] = counts[i] + extra
            spare = spare - extra
    return np.array([bound] + counts)


def ragged(rng, number_of, total, bound, slope):
    if number_of == 2:
        one = jax.random.randint(rng, (), max(1, total - bound), min(bound, total - 1) + 1)
        return jnp.stack([one, total - one])
    tallies = jnp.asarray(profile(number_of, total, bound, slope), jnp.int32)
    pairs = (number_of - 1) // 2
    giver, sink = tallies[1:1 + 2 * pairs:2], tallies[2:2 + 2 * pairs:2]
    room = jnp.minimum(giver - 1, bound - sink)
    shifted = jax.random.randint(jax.random.fold_in(rng, 1), (pairs,), 0, 1 << 20) % (room + 1)
    tallies = tallies.at[1:1 + 2 * pairs:2].set(giver - shifted).at[2:2 + 2 * pairs:2].set(sink + shifted)
    return tallies[jax.random.permutation(jax.random.fold_in(rng, 2), number_of)]


def noise(own_key, extent, spread, most, pieces=(), kind=jnp.bfloat16):
    result = spread * jax.random.normal(own_key, extent, jnp.float32)
    if pieces:
        result = result * steps_of(own_key, extent, pieces, -0.22, 0.18)
    return jnp.clip(result, -most, most).astype(kind)


def setup_inputs(seed: int = 0) -> dict:
    splits = jax.random.split(jax.random.key(seed), 6)
    tokens = noise(splits[0], (TOKENS, D), 1.0, 6.0, ((0, 16), (1, 8)))
    ref_qkv = noise(splits[1], (D, (QH + 2 * KVH) * HD), D ** -0.5, 0.078125, ((0, 128), (1, 8)))
    ref_bias = draw_ref_bias(jax.random.fold_in(splits[5], 71), 0)
    segment_ids = jax.vmap(lambda own: jnp.searchsorted(jnp.cumsum(ragged(own, max(3, TOK_DEV // 128), TOK_DEV, TOK_DEV // 2, 2)), jnp.arange(TOK_DEV), side="right"))(jax.random.split(splits[3], N_FSDP)).reshape((N_FSDP, TOK_DEV)).astype(jnp.int32)
    policy_key = noise(splits[4], (D, KVH * HD), D ** -0.5, 0.078125, ((0, 128), (1, 8)))
    return {"tokens": tokens, "ref_qkv": ref_qkv, "ref_bias": ref_bias, "segment_ids": segment_ids, "policy_key": policy_key}


def positions_of(seg):
    count = seg.shape[0]
    index = jnp.arange(count, dtype=jnp.int32)
    starts = jnp.concatenate([jnp.ones((1,), bool), seg[1:] != seg[:-1]])
    first = lax.cummax(jnp.where(starts, index, 0).astype(jnp.int32), axis=0)
    return (index - first).astype(jnp.int32)

def rotary(values, pos):
    half = values.shape[-1] // 2
    freq = 1000000.0 ** (-2.0 * jnp.arange(half, dtype=jnp.float32) / values.shape[-1])
    angle = pos.astype(jnp.float32)[:, None] * freq[None, :]
    shape = (values.shape[0],) + (1,) * (values.ndim - 2) + (half,)
    cosine = jnp.cos(angle).reshape(shape)
    sine = jnp.sin(angle).reshape(shape)
    first = values[..., :half]
    second = values[..., half:]
    return jnp.concatenate([first * cosine - second * sine, second * cosine + first * sine], axis=-1)

def reference(tokens, ref_qkv, ref_bias, segment_ids, policy_key):
    share = QH // KVH
    proj = jnp.dot(tokens, ref_qkv, preferred_element_type=jnp.float32) + ref_bias[None, :]
    proj = proj.reshape(N_FSDP, TOK_DEV, KVH, share + 2, HD)

    def one_pack(args):
        block, seg = args
        pos = positions_of(seg)
        query = rotary(block[:, :, :share], pos).astype(jnp.bfloat16)
        keys = rotary(block[:, :, share], pos).astype(jnp.bfloat16)
        vals = block[:, :, share + 1].astype(jnp.bfloat16)
        scores = jnp.einsum('qhgd,khd->hgqk', query.astype(jnp.float32), keys.astype(jnp.float32)) / jnp.sqrt(jnp.float32(HD))
        index = jnp.arange(TOK_DEV)
        allowed = (seg[:, None] == seg[None, :]) & (index[None, :] <= index[:, None])
        scores = jnp.where(allowed[None, None], scores, -1e+30)
        top = lax.optimization_barrier(jnp.max(scores, axis=-1, keepdims=True))
        expo = jnp.exp(scores - top)
        weights = (expo / lax.optimization_barrier(jnp.sum(expo, axis=-1, keepdims=True))).astype(jnp.bfloat16)
        ctx = jnp.einsum('hgqk,khd->qhgd', weights.astype(jnp.float32), vals.astype(jnp.float32))
        return ctx.astype(jnp.bfloat16).reshape(TOK_DEV, QH * HD)
    context = lax.map(one_pack, (proj, segment_ids))
    return (context.reshape(TOKENS, QH * HD), policy_key)
```

```python
import jax
import jax.numpy as jnp
from jax import lax
from jax.experimental import pallas as pl
from jax.experimental.pallas import tpu as pltpu
from jax.sharding import PartitionSpec as P

QH = 40
KVH = 8
HD = 128
HALF = HD // 2
SHARE = QH // KVH
WINDOW = 5


def copies_of(array, count):
    return jnp.broadcast_to(array, (count, *array.shape))


def exchanged(blocks, axis):
    return lax.all_to_all(blocks, axis, split_axis=0, concat_axis=0, tiled=True)


def cost(flops, moved):
    return pl.CostEstimate(flops=flops, bytes_accessed=moved, transcendentals=0)


def call(kernel, outs, flops, *args, scalars=0):
    vmem = pl.BlockSpec(memory_space=pltpu.VMEM)
    smem = pl.BlockSpec(memory_space=pltpu.SMEM)
    moved = sum(a.size * a.dtype.itemsize for a in (*args, *outs))
    return pl.pallas_call(
        kernel,
        out_shape=outs if len(outs) > 1 else outs[0],
        in_specs=[smem] * scalars + [vmem] * (len(args) - scalars),
        out_specs=tuple(vmem for _ in outs) if len(outs) > 1 else vmem,
        compiler_params=pltpu.CompilerParams(vmem_limit_bytes=24 * 1024 * 1024),
        cost_estimate=cost(flops, moved),
    )(*args)


def lanes_below_half(shape):
    return lax.broadcasted_iota(jnp.int32, shape, len(shape) - 1) < HALF


def project(own_ref, other_ref, w_ref, kv_ref, q_ref):
    blocks = kv_ref.shape[0]
    rows = own_ref.shape[0]
    step = rows // 2
    shared = w_ref[:, 3 * HD : 4 * HD]
    w_own = w_ref[:, : 4 * HD]
    swapped = pltpu.roll(shared.astype(jnp.float32), HALF, 1).astype(jnp.bfloat16)
    w_other = jnp.concatenate([w_ref[:, 4 * HD :], swapped], axis=1)
    size = rows // blocks
    low = lanes_below_half((size // 2, HD))
    for part in range(2):
        at = part * step
        own = own_ref[at : at + step, :]
        other = other_ref[at : at + step, :]
        value = jnp.dot(own, w_own, preferred_element_type=jnp.float32)
        value = value + jnp.dot(other, w_other, preferred_element_type=jnp.float32)
        for b in range(step // size):
            j = at // size + b
            piece = value[b * size : (b + 1) * size]
            kv_ref[j] = piece[:, :HD].astype(jnp.bfloat16)
            q_ref[j, :size] = piece[:, HD : 2 * HD].astype(jnp.bfloat16)
            q_ref[j, size : 2 * size] = piece[:, 2 * HD : 3 * HD].astype(jnp.bfloat16)
            last = piece[:, 3 * HD :]
            packed = jnp.where(low, last[: size // 2], pltpu.roll(last[size // 2 :], HALF, 1))
            q_ref[j, 2 * size :] = packed.astype(jnp.bfloat16)


def turned(value, cosine, sine):
    return value * cosine + pltpu.roll(value, HALF, 1) * sine


def added(ref, parity, rows):
    value = ref[parity, rows].astype(jnp.float32)
    for j in range(parity + 2, ref.shape[0], 2):
        value = value + ref[j, rows].astype(jnp.float32)
    return value


def keys_and_values(part_ref, bias_ref, cos_ref, sin_ref, out_ref):
    size = part_ref.shape[1]
    every = slice(0, size)
    key = added(part_ref, 0, every) + bias_ref[SHARE : SHARE + 1]
    key = turned(key, cos_ref[...], sin_ref[...]).astype(jnp.bfloat16)
    val = (added(part_ref, 1, every) + bias_ref[SHARE + 1 : SHARE + 2]).astype(jnp.bfloat16)
    for j in range(out_ref.shape[0]):
        out_ref[j, :size] = key
        out_ref[j, size:] = val


def attend(rank_ref, part_ref, kv_ref, bias_ref, cos_ref, sin_ref, seg_ref, mine_ref, out_ref):
    size = out_ref.shape[0]
    blocks = kv_ref.shape[0]
    window = min(WINDOW, blocks)
    rank = rank_ref[0]
    first = jnp.clip(rank - (window - 1), 0, blocks - window)
    low = lanes_below_half((size // 2, HD))
    left = added(part_ref, 0, slice(2 * size, 5 * size // 2))
    right = added(part_ref, 1, slice(2 * size, 5 * size // 2))
    middle = jnp.concatenate(
        [
            jnp.where(low, left, pltpu.roll(right, HALF, 1)),
            jnp.where(low, pltpu.roll(left, HALF, 1), right),
        ],
        axis=0,
    )
    heads = [
        added(part_ref, 0, slice(0, size)),
        added(part_ref, 0, slice(size, 2 * size)),
        middle,
        added(part_ref, 1, slice(0, size)),
        added(part_ref, 1, slice(size, 2 * size)),
    ]
    span = kv_ref[pl.ds(first, window)]
    keys = span[:, :size].reshape(window * size, HD)
    vals = span[:, size:].reshape(window * size, HD)
    row = rank * size + lax.broadcasted_iota(jnp.int32, (size, size), 0)
    lane = lax.broadcasted_iota(jnp.int32, (size, size), 1)
    masks = []
    for b in range(window):
        seg = seg_ref[pl.ds(first + b, 1), :]
        column = (first + b) * size + lane
        masks.append((mine_ref[...] == seg) & (column <= row))
    allowed = jnp.concatenate(masks, axis=1)
    cosine, sine = cos_ref[...], sin_ref[...]
    for h in range(SHARE):
        query = turned(heads[h] + bias_ref[h : h + 1], cosine, sine).astype(jnp.bfloat16)
        scores = lax.dot_general(
            query, keys, (((1,), (1,)), ((), ())), preferred_element_type=jnp.float32
        )
        scores = jnp.where(allowed, scores / jnp.sqrt(jnp.float32(HD)), -1e30)
        top = jnp.max(scores, axis=-1, keepdims=True)
        expo = jnp.exp(scores - top)
        weights = (expo / jnp.sum(expo, axis=-1, keepdims=True)).astype(jnp.bfloat16)
        context = jnp.dot(weights, vals, preferred_element_type=jnp.float32)
        out_ref[:, h * HD : (h + 1) * HD] = context.astype(jnp.bfloat16)


def per_device(tokens, ref_qkv, ref_bias, segment_ids, policy_key):
    replicas = lax.axis_size("rep")
    shards = lax.axis_size("fsdp")
    rows, features = tokens.shape
    mine = rows // replicas
    rank = lax.axis_index("rep")
    odd = (rank & 1) == 1
    swap = [(i, i ^ 1) for i in range(replicas)]
    bf16, f32 = jnp.bfloat16, jnp.float32

    w = ref_qkv
    kv = (w[:, 5 * HD : 6 * HD], w[:, 6 * HD :])
    wide = (w[:, : 2 * HD], w[:, 3 * HD : 5 * HD])
    thin = (w[:, 2 * HD : 2 * HD + HALF], w[:, 2 * HD + HALF : 3 * HD])
    keep = jnp.where(
        odd,
        jnp.concatenate([kv[1], wide[1], thin[1]], axis=1),
        jnp.concatenate([kv[0], wide[0], thin[0]], axis=1),
    )
    give = jnp.where(
        odd,
        jnp.concatenate([thin[0], kv[0], wide[0]], axis=1),
        jnp.concatenate([thin[1], kv[1], wide[1]], axis=1),
    )
    with jax.named_scope("w_swap"):
        got = lax.ppermute(give, "rep", swap)
    with jax.named_scope("t_swap"):
        other = lax.ppermute(tokens, "rep", swap)
    mixed = jnp.concatenate([keep, got], axis=1)
    with jax.named_scope("w_gather"):
        weights = exchanged(copies_of(mixed, shards), "fsdp").reshape(features, -1)

    with jax.named_scope("pol_rep"):
        inner = exchanged(copies_of(policy_key, replicas), "rep")
    blocks, width = policy_key.shape
    with jax.named_scope("pol_fsdp"):
        outer = exchanged(copies_of(inner.reshape(replicas * blocks, width), shards), "fsdp")
    whole = (
        outer.reshape(shards, replicas, blocks, width)
        .transpose(1, 0, 2, 3)
        .reshape(shards * replicas * blocks, width)
    )

    seg = segment_ids[0]
    start = rank * mine
    my_seg = lax.dynamic_slice_in_dim(seg, start, mine, 0)
    before = jnp.sum((seg[None, :] < my_seg[:, None]).astype(jnp.int32), axis=1)
    pos = start + jnp.arange(mine, dtype=jnp.int32) - before
    freq = 1000000.0 ** (-2.0 * jnp.arange(HALF, dtype=f32) / HD)
    angle = pos.astype(f32)[:, None] * freq[None, :]
    cosine, sine = jnp.cos(angle), jnp.sin(angle)
    cosine = jnp.concatenate([cosine, cosine], axis=1)
    sine = jnp.concatenate([-sine, sine], axis=1)
    bias = ref_bias.reshape(SHARE + 2, HD)

    part_kv, part_q = call(
        project,
        (
            jax.ShapeDtypeStruct((replicas, mine, HD), bf16),
            jax.ShapeDtypeStruct((replicas, 5 * mine // 2, HD), bf16),
        ),
        4 * rows * features * 4 * HD,
        tokens,
        other,
        weights,
    )
    with jax.named_scope("kv_sum"):
        part_kv = exchanged(part_kv, "rep")
    with jax.named_scope("q_sum"):
        part_q = exchanged(part_q, "rep")
    my_kv = call(
        keys_and_values,
        (jax.ShapeDtypeStruct((replicas, 2 * mine, HD), bf16),),
        16 * mine * HD,
        part_kv,
        bias,
        cosine,
        sine,
    )
    with jax.named_scope("kv_gather"):
        all_kv = exchanged(my_kv, "rep")
    context = call(
        attend,
        (jax.ShapeDtypeStruct((mine, SHARE * HD), bf16),),
        4 * SHARE * mine * WINDOW * mine * HD,
        rank.reshape(1),
        part_q,
        all_kv,
        bias,
        cosine,
        sine,
        seg.reshape(replicas, mine),
        my_seg[:, None],
        scalars=1,
    )
    return (context, whole)


def solution(mesh):
    in_specs = (
        P("fsdp", "rep"),
        P(("rep", "fsdp"), "tp"),
        P("tp"),
        P("fsdp", None),
        P(("rep", "fsdp"), "tp"),
    )
    out_specs = (P(("fsdp", "rep"), "tp"), P(None, "tp"))
    return jax.shard_map(
        per_device, mesh=mesh, in_specs=in_specs, out_specs=out_specs, check_vma=False
    )
```

```python
import jax
import jax.numpy as jnp
from jax import lax
from jax.experimental import pallas as pl
from jax.experimental.pallas import tpu as pltpu
from jax.sharding import PartitionSpec as P

QH = 40
KVH = 8
HD = 128
HALF = HD // 2
SHARE = QH // KVH
WINDOW = 5


def copies_of(array, count):
    return jnp.broadcast_to(array, (count, *array.shape))


def exchanged(blocks, axis):
    return lax.all_to_all(blocks, axis, split_axis=0, concat_axis=0, tiled=True)


def cost(flops, moved):
    return pl.CostEstimate(flops=flops, bytes_accessed=moved, transcendentals=0)


def call(kernel, outs, flops, *args, scalars=0):
    vmem = pl.BlockSpec(memory_space=pltpu.VMEM)
    smem = pl.BlockSpec(memory_space=pltpu.SMEM)
    moved = sum(a.size * a.dtype.itemsize for a in (*args, *outs))
    return pl.pallas_call(
        kernel,
        out_shape=outs if len(outs) > 1 else outs[0],
        in_specs=[smem] * scalars + [vmem] * (len(args) - scalars),
        out_specs=tuple(vmem for _ in outs) if len(outs) > 1 else vmem,
        compiler_params=pltpu.CompilerParams(vmem_limit_bytes=24 * 1024 * 1024),
        cost_estimate=cost(flops, moved),
    )(*args)


def project(tokens_ref, w_hbm, kv_ref, q_ref, w_ref, sem):
    load = pltpu.make_async_copy(w_hbm, w_ref, sem)
    load.start()
    load.wait()
    blocks = kv_ref.shape[0]
    rows = tokens_ref.shape[0]
    size = rows // blocks
    step = rows // 2
    for part in range(2):
        at = part * step
        own = tokens_ref[at : at + step, :]
        value = jnp.dot(own, w_ref[:, SHARE * HD :], preferred_element_type=jnp.float32)
        value = value.astype(jnp.bfloat16)
        for b in range(step // size):
            j = at // size + b
            kv_ref[j, :size] = value[b * size : (b + 1) * size, :HD]
            kv_ref[j, size:] = value[b * size : (b + 1) * size, HD:]
        value = jnp.dot(own, w_ref[:, : SHARE * HD], preferred_element_type=jnp.float32)
        q_ref[at : at + step, :] = value.astype(jnp.bfloat16)


def projected(tokens, weights, blocks):
    rows, features = tokens.shape
    vmem = pl.BlockSpec(memory_space=pltpu.VMEM)
    return pl.pallas_call(
        project,
        out_shape=(
            jax.ShapeDtypeStruct((blocks, 2 * rows // blocks, HD), jnp.bfloat16),
            jax.ShapeDtypeStruct((rows, SHARE * HD), jnp.bfloat16),
        ),
        in_specs=[vmem, pl.BlockSpec(memory_space=pltpu.HBM)],
        out_specs=(vmem, vmem),
        scratch_shapes=[pltpu.VMEM(weights.shape, weights.dtype), pltpu.SemaphoreType.DMA],
        compiler_params=pltpu.CompilerParams(vmem_limit_bytes=60 * 1024 * 1024),
        cost_estimate=cost(2 * rows * weights.size, 2 * (tokens.size + weights.size)),
    )(tokens, weights)


def turned(value, cosine, sine):
    return value * cosine + pltpu.roll(value, HALF, 1) * sine


def added(ref, rows):
    value = ref[0, rows].astype(jnp.float32)
    for j in range(1, ref.shape[0]):
        value = value + ref[j, rows].astype(jnp.float32)
    return value


def keys_and_values(part_ref, bias_ref, cos_ref, sin_ref, out_ref):
    size = part_ref.shape[1] // 2
    key = added(part_ref, slice(0, size)) + bias_ref[SHARE : SHARE + 1]
    key = turned(key, cos_ref[...], sin_ref[...]).astype(jnp.bfloat16)
    val = added(part_ref, slice(size, 2 * size)) + bias_ref[SHARE + 1 : SHARE + 2]
    val = val.astype(jnp.bfloat16)
    for j in range(out_ref.shape[0]):
        out_ref[j, :size] = key
        out_ref[j, size:] = val


def attend(rank_ref, q_ref, kv_ref, bias_ref, cos_ref, sin_ref, seg_ref, mine_ref, out_ref):
    size = out_ref.shape[0]
    blocks = kv_ref.shape[0]
    window = min(WINDOW, blocks)
    rank = rank_ref[0]
    first = jnp.clip(rank - (window - 1), 0, blocks - window)
    span = kv_ref[pl.ds(first, window)]
    keys = span[:, :size].reshape(window * size, HD)
    vals = span[:, size:].reshape(window * size, HD)
    row = rank * size + lax.broadcasted_iota(jnp.int32, (size, size), 0)
    lane = lax.broadcasted_iota(jnp.int32, (size, size), 1)
    masks = []
    for b in range(window):
        seg = seg_ref[pl.ds(first + b, 1), :]
        column = (first + b) * size + lane
        masks.append((mine_ref[...] == seg) & (column <= row))
    allowed = jnp.concatenate(masks, axis=1)
    cosine, sine = cos_ref[...], sin_ref[...]
    for h in range(SHARE):
        query = q_ref[:, h * HD : (h + 1) * HD].astype(jnp.float32) + bias_ref[h : h + 1]
        query = turned(query, cosine, sine).astype(jnp.bfloat16)
        scores = lax.dot_general(
            query, keys, (((1,), (1,)), ((), ())), preferred_element_type=jnp.float32
        )
        scores = jnp.where(allowed, scores / jnp.sqrt(jnp.float32(HD)), -1e30)
        top = jnp.max(scores, axis=-1, keepdims=True)
        expo = jnp.exp(scores - top)
        weights = (expo / jnp.sum(expo, axis=-1, keepdims=True)).astype(jnp.bfloat16)
        context = jnp.dot(weights, vals, preferred_element_type=jnp.float32)
        out_ref[:, h * HD : (h + 1) * HD] = context.astype(jnp.bfloat16)


def per_device(tokens, ref_qkv, ref_bias, segment_ids, policy_key):
    replicas = lax.axis_size("rep")
    shards = lax.axis_size("fsdp")
    rows, features = tokens.shape
    mine = rows // replicas
    rank = lax.axis_index("rep")
    bf16, f32 = jnp.bfloat16, jnp.float32

    with jax.named_scope("w_gather"):
        weights = exchanged(copies_of(ref_qkv, shards), "fsdp").reshape(features, -1)
    blocks, width = policy_key.shape
    with jax.named_scope("pol_rep"):
        inner = exchanged(copies_of(policy_key, replicas), "rep").reshape(-1, width)
    with jax.named_scope("pol_fsdp"):
        outer = lax.all_gather(inner, "fsdp", axis=0, tiled=True)
    whole = (
        outer.reshape(shards, replicas, blocks, width)
        .transpose(1, 0, 2, 3)
        .reshape(shards * replicas * blocks, width)
    )

    seg = segment_ids[0]
    start = rank * mine
    my_seg = lax.dynamic_slice_in_dim(seg, start, mine, 0)
    before = jnp.sum((seg[None, :] < my_seg[:, None]).astype(jnp.int32), axis=1)
    pos = start + jnp.arange(mine, dtype=jnp.int32) - before
    freq = 1000000.0 ** (-2.0 * jnp.arange(HALF, dtype=f32) / HD)
    angle = pos.astype(f32)[:, None] * freq[None, :]
    cosine, sine = jnp.cos(angle), jnp.sin(angle)
    cosine = jnp.concatenate([cosine, cosine], axis=1)
    sine = jnp.concatenate([-sine, sine], axis=1)
    bias = ref_bias.reshape(SHARE + 2, HD)

    part_kv, part_q = projected(tokens, weights, replicas)
    with jax.named_scope("q_sum"):
        my_q = lax.psum_scatter(part_q, "rep", scatter_dimension=0, tiled=True)
    with jax.named_scope("kv_sum"):
        part_kv = exchanged(part_kv, "rep")
    my_kv = call(
        keys_and_values,
        (jax.ShapeDtypeStruct((replicas, 2 * mine, HD), bf16),),
        32 * mine * HD,
        part_kv,
        bias,
        cosine,
        sine,
    )
    with jax.named_scope("kv_gather"):
        all_kv = exchanged(my_kv, "rep")
    context = call(
        attend,
        (jax.ShapeDtypeStruct((mine, SHARE * HD), bf16),),
        4 * SHARE * mine * WINDOW * mine * HD,
        rank.reshape(1),
        my_q,
        all_kv,
        bias,
        cosine,
        sine,
        seg.reshape(replicas, mine),
        my_seg[:, None],
        scalars=1,
    )
    return (context, whole)


def solution(mesh):
    in_specs = (
        P("fsdp", "rep"),
        P(("rep", "fsdp"), "tp"),
        P("tp"),
        P("fsdp", None),
        P(("rep", "fsdp"), "tp"),
    )
    out_specs = (P(("fsdp", "rep"), "tp"), P(None, "tp"))
    return jax.shard_map(
        per_device, mesh=mesh, in_specs=in_specs, out_specs=out_specs, check_vma=False
    )
```

```python
import jax
import jax.numpy as jnp
from jax import lax
from jax.experimental import pallas as pl
from jax.experimental.pallas import tpu as pltpu
from jax.sharding import PartitionSpec as P


QH = 40
KVH = 8
HD = 128
HALF = HD // 2
SHARE = QH // KVH
WINDOW = 5


def copies_of(array, count):
    return jnp.broadcast_to(array, (count, *array.shape))


def exchanged(blocks, axis):
    return lax.all_to_all(blocks, axis, split_axis=0, concat_axis=0, tiled=True)


def cost(flops, moved):
    return pl.CostEstimate(flops=flops, bytes_accessed=moved, transcendentals=0)


def call(kernel, outs, flops, *args, scalars=0):
    vmem = pl.BlockSpec(memory_space=pltpu.VMEM)
    smem = pl.BlockSpec(memory_space=pltpu.SMEM)
    moved = sum(a.size * a.dtype.itemsize for a in (*args, *outs))
    return pl.pallas_call(
        kernel,
        out_shape=outs if len(outs) > 1 else outs[0],
        in_specs=[smem] * scalars + [vmem] * (len(args) - scalars),
        out_specs=tuple(vmem for _ in outs) if len(outs) > 1 else vmem,
        compiler_params=pltpu.CompilerParams(vmem_limit_bytes=24 * 1024 * 1024),
        cost_estimate=cost(flops, moved),
    )(*args)


def lanes_below_half(shape):
    return lax.broadcasted_iota(jnp.int32, shape, len(shape) - 1) < HALF


def split(rank_ref, w_ref, keep_ref, give_ref):
    key, val = w_ref[:, 5 * HD : 6 * HD], w_ref[:, 6 * HD :]
    low, high = w_ref[:, : 2 * HD], w_ref[:, 3 * HD : 5 * HD]
    left, right = w_ref[:, 2 * HD : 2 * HD + HALF], w_ref[:, 2 * HD + HALF : 3 * HD]
    odd = jnp.bitwise_and(rank_ref[0], 1)

    @pl.when(odd == 0)
    def _():
        keep_ref[...] = jnp.concatenate([key, low, left], axis=1)
        give_ref[...] = jnp.concatenate([right, val, high], axis=1)

    @pl.when(odd == 1)
    def _():
        keep_ref[...] = jnp.concatenate([val, high, right], axis=1)
        give_ref[...] = jnp.concatenate([left, key, low], axis=1)


def pack(keep_ref, got_ref, inner_ref, out_ref):
    parts = [keep_ref[...], got_ref[...]] + [inner_ref[j] for j in range(inner_ref.shape[0])]
    row = jnp.concatenate(parts, axis=1)
    for j in range(out_ref.shape[0]):
        out_ref[j] = row


def arrange(in_ref, out_ref):
    out_ref[0] = in_ref[...]


def arranged(gathered, replicas, width):
    rows = gathered.shape[0]
    first = 7 * HD // width
    return pl.pallas_call(
        arrange,
        grid=(replicas,),
        out_shape=jax.ShapeDtypeStruct((replicas, rows, width), gathered.dtype),
        in_specs=[pl.BlockSpec((rows, width), lambda j: (0, first + j))],
        out_specs=pl.BlockSpec((1, rows, width), lambda j: (j, 0, 0)),
        compiler_params=pltpu.CompilerParams(vmem_limit_bytes=8 * 1024 * 1024),
        cost_estimate=cost(0, 4 * replicas * rows * width),
    )(gathered)


def project(own_hbm, other_hbm, w_hbm, out_ref, own_ref, other_ref, w_ref, sems):
    blocks = out_ref.shape[0]
    rows = own_hbm.shape[0]
    step = rows // 2
    loads = [pltpu.make_async_copy(w_hbm.at[:, : 7 * HD], w_ref, sems.at[0])]
    for part in range(2):
        span = pl.ds(part * step, step)
        loads.append(pltpu.make_async_copy(own_hbm.at[span], own_ref.at[span], sems.at[1 + 2 * part]))
        loads.append(
            pltpu.make_async_copy(other_hbm.at[span], other_ref.at[span], sems.at[2 + 2 * part])
        )
    for load in loads:
        load.start()
    loads[0].wait()
    shared = w_ref[:, 3 * HD : 4 * HD]
    w_own = w_ref[:, : 4 * HD]
    swapped = pltpu.roll(shared.astype(jnp.float32), HALF, 1).astype(jnp.bfloat16)
    w_other = jnp.concatenate([w_ref[:, 4 * HD :], swapped], axis=1)
    size = rows // blocks
    low = lanes_below_half((size // 2, HD))
    for part in range(2):
        loads[1 + 2 * part].wait()
        loads[2 + 2 * part].wait()
        at = part * step
        value = jnp.dot(own_ref[at : at + step, :], w_own, preferred_element_type=jnp.float32)
        value = value + jnp.dot(
            other_ref[at : at + step, :], w_other, preferred_element_type=jnp.float32
        )
        for b in range(step // size):
            j = at // size + b
            piece = value[b * size : (b + 1) * size]
            for c in range(3):
                out_ref[j, c * size : (c + 1) * size] = piece[:, c * HD : (c + 1) * HD].astype(
                    jnp.bfloat16
                )
            last = piece[:, 3 * HD :]
            packed = jnp.where(low, last[: size // 2], pltpu.roll(last[size // 2 :], HALF, 1))
            out_ref[j, 3 * size :] = packed.astype(jnp.bfloat16)


def projected(own, other, gathered, blocks):
    rows, features = own.shape
    vmem = pl.BlockSpec(memory_space=pltpu.VMEM)
    hbm = pl.BlockSpec(memory_space=pltpu.HBM)
    return pl.pallas_call(
        project,
        out_shape=jax.ShapeDtypeStruct((blocks, 7 * rows // blocks // 2, HD), jnp.bfloat16),
        in_specs=[hbm, hbm, hbm],
        out_specs=vmem,
        scratch_shapes=[
            pltpu.VMEM(own.shape, own.dtype),
            pltpu.VMEM(own.shape, own.dtype),
            pltpu.VMEM((features, 7 * HD), own.dtype),
            pltpu.SemaphoreType.DMA((5,)),
        ],
        compiler_params=pltpu.CompilerParams(vmem_limit_bytes=62 * 1024 * 1024),
        cost_estimate=cost(4 * rows * features * 4 * HD, 4 * own.size + 2 * gathered.size),
    )(own, other, gathered)


def turned(value, cosine, sine):
    return value * cosine + pltpu.roll(value, HALF, 1) * sine


def added(ref, parity, rows):
    value = ref[parity, rows].astype(jnp.float32)
    for j in range(parity + 2, ref.shape[0], 2):
        value = value + ref[j, rows].astype(jnp.float32)
    return value


def keys_and_values(part_ref, bias_ref, cos_ref, sin_ref, out_ref):
    size = out_ref.shape[1] // 2
    rows = slice(0, size)
    key = added(part_ref, 0, rows) + bias_ref[SHARE : SHARE + 1]
    key = turned(key, cos_ref[...], sin_ref[...]).astype(jnp.bfloat16)
    val = (added(part_ref, 1, rows) + bias_ref[SHARE + 1 : SHARE + 2]).astype(jnp.bfloat16)
    for j in range(out_ref.shape[0]):
        out_ref[j, :size] = key
        out_ref[j, size:] = val


def attend(rank_ref, part_ref, kv_ref, bias_ref, cos_ref, sin_ref, seg_ref, mine_ref, out_ref):
    size = out_ref.shape[0]
    blocks = kv_ref.shape[0]
    window = min(WINDOW, blocks)
    rank = rank_ref[0]
    first = jnp.clip(rank - (window - 1), 0, blocks - window)
    low = lanes_below_half((size // 2, HD))
    left = added(part_ref, 0, slice(3 * size, 7 * size // 2))
    right = added(part_ref, 1, slice(3 * size, 7 * size // 2))
    middle = jnp.concatenate(
        [
            jnp.where(low, left, pltpu.roll(right, HALF, 1)),
            jnp.where(low, pltpu.roll(left, HALF, 1), right),
        ],
        axis=0,
    )
    heads = [
        added(part_ref, 0, slice(size, 2 * size)),
        added(part_ref, 0, slice(2 * size, 3 * size)),
        middle,
        added(part_ref, 1, slice(size, 2 * size)),
        added(part_ref, 1, slice(2 * size, 3 * size)),
    ]
    span = kv_ref[pl.ds(first, window)]
    keys = span[:, :size].reshape(window * size, HD)
    vals = span[:, size:].reshape(window * size, HD)
    row = rank * size + lax.broadcasted_iota(jnp.int32, (size, size), 0)
    lane = lax.broadcasted_iota(jnp.int32, (size, size), 1)
    masks = []
    for b in range(window):
        seg = seg_ref[pl.ds(first + b, 1), :]
        column = (first + b) * size + lane
        masks.append((mine_ref[...] == seg) & (column <= row))
    allowed = jnp.concatenate(masks, axis=1)
    cosine, sine = cos_ref[...], sin_ref[...]
    for h in range(SHARE):
        query = turned(heads[h] + bias_ref[h : h + 1], cosine, sine).astype(jnp.bfloat16)
        scores = lax.dot_general(
            query, keys, (((1,), (1,)), ((), ())), preferred_element_type=jnp.float32
        )
        scores = jnp.where(allowed, scores / jnp.sqrt(jnp.float32(HD)), -1e30)
        top = jnp.max(scores, axis=-1, keepdims=True)
        expo = jnp.exp(scores - top)
        weights = (expo / jnp.sum(expo, axis=-1, keepdims=True)).astype(jnp.bfloat16)
        context = jnp.dot(weights, vals, preferred_element_type=jnp.float32)
        out_ref[:, h * HD : (h + 1) * HD] = context.astype(jnp.bfloat16)


def body(tokens, ref_qkv, ref_bias, segment_ids, policy_key):
    replicas = lax.axis_size("rep")
    shards = lax.axis_size("fsdp")
    rows, features = tokens.shape
    mine = rows // replicas
    rank = lax.axis_index("rep")
    swap = [(i, i ^ 1) for i in range(replicas)]
    bf16, f32 = jnp.bfloat16, jnp.float32

    own_features = ref_qkv.shape[0]
    half = jax.ShapeDtypeStruct((own_features, 7 * HALF), bf16)
    keep, give = call(split, (half, half), 0, rank.reshape(1), ref_qkv, scalars=1)
    got = lax.ppermute(give, "rep", swap)
    other = lax.ppermute(tokens, "rep", swap)
    width = policy_key.shape[1]
    inner = exchanged(copies_of(policy_key, replicas), "rep")
    packed = jax.ShapeDtypeStruct((shards, own_features, 7 * HD + replicas * width), bf16)
    packed = call(pack, (packed,), 0, keep, got, inner)
    gathered = exchanged(packed, "fsdp").reshape(features, -1)
    whole = arranged(gathered, replicas, width).reshape(-1, width)

    seg = segment_ids[0]
    start = rank * mine
    my_seg = lax.dynamic_slice_in_dim(seg, start, mine, 0)
    before = jnp.sum((seg[None, :] < my_seg[:, None]).astype(jnp.int32), axis=1)
    pos = start + jnp.arange(mine, dtype=jnp.int32) - before
    freq = 1000000.0 ** (-2.0 * jnp.arange(HALF, dtype=f32) / HD)
    angle = pos.astype(f32)[:, None] * freq[None, :]
    cosine, sine = jnp.cos(angle), jnp.sin(angle)
    cosine = jnp.concatenate([cosine, cosine], axis=1)
    sine = jnp.concatenate([-sine, sine], axis=1)
    bias = ref_bias.reshape(SHARE + 2, HD)

    part = projected(tokens, other, gathered, replicas)
    part = exchanged(part, "rep")
    my_kv = call(
        keys_and_values,
        (jax.ShapeDtypeStruct((replicas, 2 * mine, HD), bf16),),
        16 * mine * HD,
        part,
        bias,
        cosine,
        sine,
    )
    all_kv = exchanged(my_kv, "rep")
    context = call(
        attend,
        (jax.ShapeDtypeStruct((mine, SHARE * HD), bf16),),
        4 * SHARE * mine * WINDOW * mine * HD,
        rank.reshape(1),
        part,
        all_kv,
        bias,
        cosine,
        sine,
        seg.reshape(replicas, mine),
        my_seg[:, None],
        scalars=1,
    )
    return (context, whole)


def solution(mesh):
    in_specs = (
        P("fsdp", "rep"),
        P(("rep", "fsdp"), "tp"),
        P("tp"),
        P("fsdp", None),
        P(("rep", "fsdp"), "tp"),
    )
    out_specs = (P(("fsdp", "rep"), "tp"), P(None, "tp"))
    return jax.shard_map(body, mesh=mesh, in_specs=in_specs, out_specs=out_specs, check_vma=False)
```

```python
import jax
import jax.numpy as jnp
from jax import lax
from jax.experimental import pallas as pl
from jax.experimental.pallas import tpu as pltpu
from jax.sharding import PartitionSpec as P


QH = 40
KVH = 8
HD = 128
HALF = HD // 2
SHARE = QH // KVH
SIDES = 2
WINDOW = 5


def exchanged(blocks, axis):
    return lax.all_to_all(blocks, axis, split_axis=0, concat_axis=0, tiled=True)


def cost(flops, moved):
    return pl.CostEstimate(flops=flops, bytes_accessed=moved, transcendentals=0)


def call(kernel, outs, flops, *args, scalars=0):
    vmem = pl.BlockSpec(memory_space=pltpu.VMEM)
    smem = pl.BlockSpec(memory_space=pltpu.SMEM)
    moved = sum(a.size * a.dtype.itemsize for a in (*args, *outs))
    return pl.pallas_call(
        kernel,
        out_shape=outs if len(outs) > 1 else outs[0],
        in_specs=[smem] * scalars + [vmem] * (len(args) - scalars),
        out_specs=tuple(vmem for _ in outs) if len(outs) > 1 else vmem,
        compiler_params=pltpu.CompilerParams(vmem_limit_bytes=24 * 1024 * 1024),
        cost_estimate=cost(flops, moved),
    )(*args)


def lanes_below_half(shape):
    return lax.broadcasted_iota(jnp.int32, shape, len(shape) - 1) < HALF


def split(rank_ref, w_ref, policy_ref, keep_ref, give_ref):
    key, val = w_ref[:, 5 * HD : 6 * HD], w_ref[:, 6 * HD :]
    low, high = w_ref[:, : 2 * HD], w_ref[:, 3 * HD : 5 * HD]
    left, right = w_ref[:, 2 * HD : 2 * HD + HALF], w_ref[:, 2 * HD + HALF : 3 * HD]
    odd = jnp.bitwise_and(rank_ref[0], 1)

    @pl.when(odd == 0)
    def _():
        keep_ref[...] = jnp.concatenate([key, low, left], axis=1)
        give_ref[...] = jnp.concatenate([right, val, high, policy_ref[...]], axis=1)

    @pl.when(odd == 1)
    def _():
        keep_ref[...] = jnp.concatenate([val, high, right], axis=1)
        give_ref[...] = jnp.concatenate([left, key, low, policy_ref[...]], axis=1)


def pack(keep_ref, got_ref, policy_ref, out_ref, pair_ref):
    row = jnp.concatenate([keep_ref[...], got_ref[:, : 7 * HALF]], axis=1)
    for j in range(out_ref.shape[0]):
        out_ref[j] = row
    pair_ref[0] = policy_ref[...]
    pair_ref[1] = got_ref[:, 7 * HALF :]


def arrange(place_ref, *refs):
    *parts, out_ref, sem = refs
    x, y, z = place_ref[0], place_ref[1], place_ref[2]
    length, sides, replicas = len(parts), out_ref.shape[1], out_ref.shape[0]
    copies = []
    for k, part in enumerate(parts):
        distance = k if k <= length // 2 else k - length
        column = jnp.bitwise_and(x - distance, length - 1)
        for side in range(sides):
            for b in range(replicas):
                place = out_ref.at[z ^ b, y ^ side, column]
                copies.append(pltpu.make_async_copy(part.at[side, b], place, sem))
    for copy in copies:
        copy.start()
    pltpu.make_async_copy(out_ref, out_ref, sem).wait()


def arranged(place, parts):
    sides, replicas, rows, width = parts[0].shape
    hbm = pl.BlockSpec(memory_space=pl.ANY)
    return pl.pallas_call(
        arrange,
        out_shape=jax.ShapeDtypeStruct((replicas, sides, len(parts), rows, width), parts[0].dtype),
        in_specs=[pl.BlockSpec(memory_space=pltpu.SMEM)] + [hbm] * len(parts),
        out_specs=hbm,
        scratch_shapes=[pltpu.SemaphoreType.DMA],
        compiler_params=pltpu.CompilerParams(vmem_limit_bytes=1024 * 1024),
        cost_estimate=cost(0, 4 * len(parts) * parts[0].size),
    )(place, *parts)


def project(own_ref, low_ref, high_ref, w_ref, out_ref):
    blocks = out_ref.shape[0]
    rows = own_ref.shape[0]
    step = rows // 2
    shared = w_ref[:, 3 * HD : 4 * HD]
    w_own = w_ref[:, : 4 * HD]
    swapped = pltpu.roll(shared.astype(jnp.float32), HALF, 1).astype(jnp.bfloat16)
    w_other = jnp.concatenate([w_ref[:, 4 * HD :], swapped], axis=1)
    size = rows // blocks
    low = lanes_below_half((size // 2, HD))
    for part in range(2):
        at = part * step
        value = jnp.dot(own_ref[at : at + step, :], w_own, preferred_element_type=jnp.float32)
        value = value + jnp.dot(
            (low_ref, high_ref)[part][...], w_other, preferred_element_type=jnp.float32
        )
        for b in range(step // size):
            j = at // size + b
            piece = value[b * size : (b + 1) * size]
            for c in range(3):
                out_ref[j, c * size : (c + 1) * size] = piece[:, c * HD : (c + 1) * HD].astype(
                    jnp.bfloat16
                )
            last = piece[:, 3 * HD :]
            packed = jnp.where(low, last[: size // 2], pltpu.roll(last[size // 2 :], HALF, 1))
            out_ref[j, 3 * size :] = packed.astype(jnp.bfloat16)


def turned(value, cosine, sine):
    return value * cosine + pltpu.roll(value, HALF, 1) * sine


def added(ref, parity, rows):
    value = ref[parity, rows].astype(jnp.float32)
    for j in range(parity + 2, ref.shape[0], 2):
        value = value + ref[j, rows].astype(jnp.float32)
    return value


def keys_and_values(part_ref, bias_ref, cos_ref, sin_ref, *rest):
    out_ref = rest[-1]
    size = out_ref.shape[1] // 2
    rows = slice(0, size)
    key = added(part_ref, 0, rows) + bias_ref[SHARE : SHARE + 1]
    key = turned(key, cos_ref[...], sin_ref[...]).astype(jnp.bfloat16)
    val = (added(part_ref, 1, rows) + bias_ref[SHARE + 1 : SHARE + 2]).astype(jnp.bfloat16)
    for j in range(out_ref.shape[0]):
        out_ref[j, :size] = key
        out_ref[j, size:] = val


def attend(rank_ref, part_ref, kv_ref, bias_ref, cos_ref, sin_ref, seg_ref, mine_ref, out_ref):
    size = out_ref.shape[0]
    blocks = kv_ref.shape[0]
    window = min(WINDOW, blocks)
    rank = rank_ref[0]
    first = jnp.clip(rank - (window - 1), 0, blocks - window)
    low = lanes_below_half((size // 2, HD))
    left = added(part_ref, 0, slice(3 * size, 7 * size // 2))
    right = added(part_ref, 1, slice(3 * size, 7 * size // 2))
    middle = jnp.concatenate(
        [
            jnp.where(low, left, pltpu.roll(right, HALF, 1)),
            jnp.where(low, pltpu.roll(left, HALF, 1), right),
        ],
        axis=0,
    )
    heads = [
        added(part_ref, 0, slice(size, 2 * size)),
        added(part_ref, 0, slice(2 * size, 3 * size)),
        middle,
        added(part_ref, 1, slice(size, 2 * size)),
        added(part_ref, 1, slice(2 * size, 3 * size)),
    ]
    span = kv_ref[pl.ds(first, window)]
    keys = span[:, :size].reshape(window * size, HD)
    vals = span[:, size:].reshape(window * size, HD)
    row = rank * size + lax.broadcasted_iota(jnp.int32, (size, size), 0)
    lane = lax.broadcasted_iota(jnp.int32, (size, size), 1)
    masks = []
    for b in range(window):
        seg = seg_ref[pl.ds(first + b, 1), :]
        column = (first + b) * size + lane
        masks.append((mine_ref[...] == seg) & (column <= row))
    allowed = jnp.concatenate(masks, axis=1)
    cosine, sine = cos_ref[...], sin_ref[...]
    for h in range(SHARE):
        query = turned(heads[h] + bias_ref[h : h + 1], cosine, sine).astype(jnp.bfloat16)
        scores = lax.dot_general(
            query, keys, (((1,), (1,)), ((), ())), preferred_element_type=jnp.float32
        )
        scores = jnp.where(allowed, scores / jnp.sqrt(jnp.float32(HD)), -1e30)
        top = jnp.max(scores, axis=-1, keepdims=True)
        expo = jnp.exp(scores - top)
        weights = (expo / jnp.sum(expo, axis=-1, keepdims=True)).astype(jnp.bfloat16)
        context = jnp.dot(weights, vals, preferred_element_type=jnp.float32)
        out_ref[:, h * HD : (h + 1) * HD] = context.astype(jnp.bfloat16)


def body(tokens, ref_qkv, ref_bias, segment_ids, policy_key):
    replicas = lax.axis_size("rep")
    shards = lax.axis_size("fsdp")
    rows, features = tokens.shape
    mine = rows // replicas
    rank = lax.axis_index("rep")
    bf16, f32 = jnp.bfloat16, jnp.float32
    length = shards // SIDES
    shard = lax.axis_index("fsdp")

    def swapped(value, axis, bit):
        pairs = [(i, i ^ bit) for i in range(lax.axis_size(axis))]
        return lax.ppermute(value, axis, pairs)

    def passed(value, by):
        pairs = [(i, i // length * length + (i + by) % length) for i in range(shards)]
        return lax.ppermute(value, "fsdp", pairs)

    own_features, width = policy_key.shape
    half = jax.ShapeDtypeStruct((own_features, 7 * HALF), bf16)
    more = jax.ShapeDtypeStruct((own_features, 7 * HALF + width), bf16)
    keep, give = call(split, (half, more), 0, rank.reshape(1), ref_qkv, policy_key, scalars=1)
    got = swapped(give, "rep", 1)
    low = swapped(tokens[: rows // 2], "rep", 1)
    copies = jax.ShapeDtypeStruct((shards, own_features, 7 * HD), bf16)
    pair = jax.ShapeDtypeStruct((2, own_features, width), bf16)
    copies, pair = call(pack, (copies, pair), 0, keep, got, policy_key)
    column = pair
    for bit in range(1, replicas.bit_length() - 1):
        column = jnp.concatenate([column, swapped(column, "rep", 1 << bit)])
    gathered = exchanged(copies, "fsdp").reshape(features, -1)
    high = swapped(tokens[rows // 2 :], "rep", 1)
    both = jnp.stack([column, swapped(column, "fsdp", length)])
    up, down = [both], [both]
    for k in range(1, length // 2 + 1):
        up.append(passed(up[-1], 1))
        if k < length // 2 or length == 1:
            down.append(passed(down[-1], -1))
    place = jnp.stack([shard % length, shard // length, rank]).astype(jnp.int32)
    whole = arranged(place, up + down[:0:-1]).reshape(-1, width)

    seg = segment_ids[0]
    start = rank * mine
    my_seg = lax.dynamic_slice_in_dim(seg, start, mine, 0)
    before = jnp.sum((seg[None, :] < my_seg[:, None]).astype(jnp.int32), axis=1)
    pos = start + jnp.arange(mine, dtype=jnp.int32) - before
    freq = 1000000.0 ** (-2.0 * jnp.arange(HALF, dtype=f32) / HD)
    angle = pos.astype(f32)[:, None] * freq[None, :]
    cosine, sine = jnp.cos(angle), jnp.sin(angle)
    cosine = jnp.concatenate([cosine, cosine], axis=1)
    sine = jnp.concatenate([-sine, sine], axis=1)
    bias = ref_bias.reshape(SHARE + 2, HD)

    part = jax.ShapeDtypeStruct((replicas, 7 * mine // 2, HD), bf16)
    part = call(project, (part,), 4 * rows * features * 4 * HD, tokens, low, high, gathered)
    part = exchanged(part, "rep")
    my_kv = call(
        keys_and_values,
        (jax.ShapeDtypeStruct((replicas, 2 * mine, HD), bf16),),
        16 * mine * HD,
        part,
        bias,
        cosine,
        sine,
    )
    all_kv = exchanged(my_kv, "rep")
    context = call(
        attend,
        (jax.ShapeDtypeStruct((mine, SHARE * HD), bf16),),
        4 * SHARE * mine * WINDOW * mine * HD,
        rank.reshape(1),
        part,
        all_kv,
        bias,
        cosine,
        sine,
        seg.reshape(replicas, mine),
        my_seg[:, None],
        scalars=1,
    )
    return (context, whole)


def solution(mesh):
    in_specs = (
        P("fsdp", "rep"),
        P(("rep", "fsdp"), "tp"),
        P("tp"),
        P("fsdp", None),
        P(("rep", "fsdp"), "tp"),
    )
    out_specs = (P(("fsdp", "rep"), "tp"), P(None, "tp"))
    return jax.shard_map(body, mesh=mesh, in_specs=in_specs, out_specs=out_specs, check_vma=False)
```

```python
import jax
import jax.numpy as jnp
from jax import lax
from jax.experimental import pallas as pl
from jax.experimental.pallas import tpu as pltpu
from jax.sharding import PartitionSpec as P


QH = 40
KVH = 8
HD = 128
HALF = HD // 2
SHARE = QH // KVH
SIDES = 2
WINDOW = 5


def exchanged(blocks, axis):
    return lax.all_to_all(blocks, axis, split_axis=0, concat_axis=0, tiled=True)


def cost(flops, moved):
    return pl.CostEstimate(flops=flops, bytes_accessed=moved, transcendentals=0)


def call(kernel, outs, flops, *args, scalars=0):
    vmem = pl.BlockSpec(memory_space=pltpu.VMEM)
    smem = pl.BlockSpec(memory_space=pltpu.SMEM)
    moved = sum(a.size * a.dtype.itemsize for a in (*args, *outs))
    return pl.pallas_call(
        kernel,
        out_shape=outs if len(outs) > 1 else outs[0],
        in_specs=[smem] * scalars + [vmem] * (len(args) - scalars),
        out_specs=tuple(vmem for _ in outs) if len(outs) > 1 else vmem,
        compiler_params=pltpu.CompilerParams(vmem_limit_bytes=24 * 1024 * 1024),
        cost_estimate=cost(flops, moved),
    )(*args)


def lanes_below_half(shape):
    return lax.broadcasted_iota(jnp.int32, shape, len(shape) - 1) < HALF


def split(rank_ref, w_hbm, policy_hbm, keep_ref, give_ref, w_ref, policy_ref, sems):
    loads = [
        pltpu.make_async_copy(w_hbm, w_ref, sems.at[0]),
        pltpu.make_async_copy(policy_hbm, policy_ref, sems.at[1]),
    ]
    for load in loads:
        load.start()
    for load in loads:
        load.wait()
    key, val = w_ref[:, 5 * HD : 6 * HD], w_ref[:, 6 * HD :]
    low, high = w_ref[:, : 2 * HD], w_ref[:, 3 * HD : 5 * HD]
    left, right = w_ref[:, 2 * HD : 2 * HD + HALF], w_ref[:, 2 * HD + HALF : 3 * HD]
    odd = jnp.bitwise_and(rank_ref[0], 1)

    @pl.when(odd == 0)
    def _():
        keep_ref[...] = jnp.concatenate([key, low, left, policy_ref[...]], axis=1)
        give_ref[...] = jnp.concatenate([right, val, high, policy_ref[...]], axis=1)

    @pl.when(odd == 1)
    def _():
        keep_ref[...] = jnp.concatenate([val, high, right, policy_ref[...]], axis=1)
        give_ref[...] = jnp.concatenate([left, key, low, policy_ref[...]], axis=1)


def split_columns(rank, w, policy):
    vmem = pl.BlockSpec(memory_space=pltpu.VMEM)
    hbm = pl.BlockSpec(memory_space=pltpu.HBM)
    rows = w.shape[0]
    return pl.pallas_call(
        split,
        out_shape=(jax.ShapeDtypeStruct((rows, 7 * HALF + policy.shape[1]), w.dtype),) * 2,
        in_specs=[pl.BlockSpec(memory_space=pltpu.SMEM), hbm, hbm],
        out_specs=(vmem, vmem),
        scratch_shapes=[
            pltpu.VMEM(w.shape, w.dtype),
            pltpu.VMEM(policy.shape, policy.dtype),
            pltpu.SemaphoreType.DMA((2,)),
        ],
        compiler_params=pltpu.CompilerParams(vmem_limit_bytes=67_000_000),
        cost_estimate=cost(0, 8 * w.size),
    )(rank.reshape(1), w, policy)


def pack(keep_ref, got_ref, out_ref, pair_ref):
    row = jnp.concatenate([keep_ref[:, : 7 * HALF], got_ref[:, : 7 * HALF]], axis=1)
    for j in range(out_ref.shape[0]):
        out_ref[j] = row
    pair_ref[0] = keep_ref[:, 7 * HALF :]
    pair_ref[1] = got_ref[:, 7 * HALF :]


def arrange(place_ref, *refs):
    *parts, out_ref, sem = refs
    x, y, z = place_ref[0], place_ref[1], place_ref[2]
    length, sides, replicas = len(parts), out_ref.shape[1], out_ref.shape[0]
    copies = []
    for k, part in enumerate(parts):
        distance = k if k <= length // 2 else k - length
        column = jnp.bitwise_and(x - distance, length - 1)
        for side in range(sides):
            for b in range(replicas):
                place = out_ref.at[z ^ b, y ^ side, column]
                copies.append(pltpu.make_async_copy(part.at[side, b], place, sem))
    for copy in copies:
        copy.start()
    pltpu.make_async_copy(out_ref, out_ref, sem).wait()


def arranged(place, parts):
    sides, replicas, rows, width = parts[0].shape
    hbm = pl.BlockSpec(memory_space=pl.ANY)
    return pl.pallas_call(
        arrange,
        out_shape=jax.ShapeDtypeStruct((replicas, sides, len(parts), rows, width), parts[0].dtype),
        in_specs=[pl.BlockSpec(memory_space=pltpu.SMEM)] + [hbm] * len(parts),
        out_specs=hbm,
        scratch_shapes=[pltpu.SemaphoreType.DMA],
        compiler_params=pltpu.CompilerParams(vmem_limit_bytes=1024 * 1024),
        cost_estimate=cost(0, 4 * len(parts) * parts[0].size),
    )(place, *parts)


def project(own_hbm, other_ref, w_ref, out_ref, own_ref, sems):
    blocks = out_ref.shape[0]
    rows = own_hbm.shape[0]
    size = rows // blocks
    step = rows // 2
    spans = [pl.ds(part * step, step) for part in range(2)]
    loads = [
        pltpu.make_async_copy(own_hbm.at[span], own_ref.at[span], sems.at[part])
        for part, span in enumerate(spans)
    ]
    for load in loads:
        load.start()
    shared = w_ref[:, 3 * HD : 4 * HD]
    w_own = w_ref[:, : 4 * HD]
    swapped = pltpu.roll(shared.astype(jnp.float32), HALF, 1).astype(jnp.bfloat16)
    w_other = jnp.concatenate([w_ref[:, 4 * HD :], swapped], axis=1)
    low = lanes_below_half((size // 2, HD))
    values = [
        jnp.dot(other_ref[span, :], w_other, preferred_element_type=jnp.float32) for span in spans
    ]
    for part in range(2):
        at = part * step
        loads[part].wait()
        value = values[part] + jnp.dot(
            own_ref[spans[part], :], w_own, preferred_element_type=jnp.float32
        )
        for b in range(step // size):
            j = at // size + b
            piece = value[b * size : (b + 1) * size]
            for c in range(3):
                out_ref[j, c * size : (c + 1) * size] = piece[:, c * HD : (c + 1) * HD].astype(
                    jnp.bfloat16
                )
            last = piece[:, 3 * HD :]
            packed = jnp.where(low, last[: size // 2], pltpu.roll(last[size // 2 :], HALF, 1))
            out_ref[j, 3 * size :] = packed.astype(jnp.bfloat16)


def projected(own, other, gathered, blocks):
    rows, features = own.shape
    vmem = pl.BlockSpec(memory_space=pltpu.VMEM)
    return pl.pallas_call(
        project,
        out_shape=jax.ShapeDtypeStruct((blocks, 7 * rows // blocks // 2, HD), jnp.bfloat16),
        in_specs=[pl.BlockSpec(memory_space=pltpu.HBM), vmem, vmem],
        out_specs=vmem,
        scratch_shapes=[pltpu.VMEM(own.shape, own.dtype), pltpu.SemaphoreType.DMA((2,))],
        compiler_params=pltpu.CompilerParams(vmem_limit_bytes=24 * 1024 * 1024),
        cost_estimate=cost(4 * rows * features * 4 * HD, 4 * own.size + 2 * gathered.size),
    )(own, other, gathered)


def turned(value, cosine, sine):
    return value * cosine + pltpu.roll(value, HALF, 1) * sine


def added(ref, parity, rows):
    value = ref[parity, rows].astype(jnp.float32)
    for j in range(parity + 2, ref.shape[0], 2):
        value = value + ref[j, rows].astype(jnp.float32)
    return value


def keys_and_values(part_ref, bias_ref, cos_ref, sin_ref, *rest):
    out_ref = rest[-1]
    size = out_ref.shape[1] // 2
    rows = slice(0, size)
    key = added(part_ref, 0, rows) + bias_ref[SHARE : SHARE + 1]
    key = turned(key, cos_ref[...], sin_ref[...]).astype(jnp.bfloat16)
    val = (added(part_ref, 1, rows) + bias_ref[SHARE + 1 : SHARE + 2]).astype(jnp.bfloat16)
    for j in range(out_ref.shape[0]):
        out_ref[j, :size] = key
        out_ref[j, size:] = val


def first_block(rank, blocks, window):
    return jnp.clip(rank - (window - 1), 0, blocks - window)


def queries(rank_ref, part_ref, bias_ref, cos_ref, sin_ref, seg_ref, mine_ref, out_ref, mask_ref):
    size = out_ref.shape[1]
    blocks = seg_ref.shape[0]
    window = mask_ref.shape[1] // size
    rank = rank_ref[0]
    first = first_block(rank, blocks, window)
    low = lanes_below_half((size // 2, HD))
    left = added(part_ref, 0, slice(3 * size, 7 * size // 2))
    right = added(part_ref, 1, slice(3 * size, 7 * size // 2))
    middle = jnp.concatenate(
        [
            jnp.where(low, left, pltpu.roll(right, HALF, 1)),
            jnp.where(low, pltpu.roll(left, HALF, 1), right),
        ],
        axis=0,
    )
    heads = [
        added(part_ref, 0, slice(size, 2 * size)),
        added(part_ref, 0, slice(2 * size, 3 * size)),
        middle,
        added(part_ref, 1, slice(size, 2 * size)),
        added(part_ref, 1, slice(2 * size, 3 * size)),
    ]
    cosine, sine = cos_ref[...], sin_ref[...]
    for h in range(SHARE):
        query = turned(heads[h] + bias_ref[h : h + 1], cosine, sine)
        out_ref[h] = query.astype(jnp.bfloat16)
    row = rank * size + lax.broadcasted_iota(jnp.int32, (size, size), 0)
    lane = lax.broadcasted_iota(jnp.int32, (size, size), 1)
    for b in range(window):
        seg = seg_ref[pl.ds(first + b, 1), :]
        allowed = (mine_ref[...] == seg) & ((first + b) * size + lane <= row)
        mask_ref[:, b * size : (b + 1) * size] = jnp.where(allowed, 0.0, -1e30)


def attend(rank_ref, q_ref, mask_ref, kv_ref, out_ref):
    size = out_ref.shape[0]
    blocks = kv_ref.shape[0]
    window = mask_ref.shape[1] // size
    first = first_block(rank_ref[0], blocks, window)
    span = kv_ref[pl.ds(first, window)]
    keys = span[:, :size].reshape(window * size, HD)
    vals = span[:, size:].reshape(window * size, HD)
    mask = mask_ref[...]
    for h in range(SHARE):
        scores = lax.dot_general(
            q_ref[h], keys, (((1,), (1,)), ((), ())), preferred_element_type=jnp.float32
        )
        scores = scores * (1.0 / HD**0.5) + mask
        top = jnp.max(scores, axis=-1, keepdims=True)
        expo = jnp.exp(scores - top)
        share = 1.0 / jnp.sum(expo, axis=-1, keepdims=True)
        weights = (expo * share).astype(jnp.bfloat16)
        context = jnp.dot(weights, vals, preferred_element_type=jnp.float32)
        out_ref[:, h * HD : (h + 1) * HD] = context.astype(jnp.bfloat16)


def body(tokens, ref_qkv, ref_bias, segment_ids, policy_key):
    replicas = lax.axis_size("rep")
    shards = lax.axis_size("fsdp")
    rows, features = tokens.shape
    mine = rows // replicas
    rank = lax.axis_index("rep")
    bf16, f32 = jnp.bfloat16, jnp.float32
    length = shards // SIDES
    shard = lax.axis_index("fsdp")

    def swapped(value, axis, bit):
        pairs = [(i, i ^ bit) for i in range(lax.axis_size(axis))]
        return lax.ppermute(value, axis, pairs)

    def passed(value, by):
        pairs = [(i, i // length * length + (i + by) % length) for i in range(shards)]
        return lax.ppermute(value, "fsdp", pairs)

    own_features, width = policy_key.shape
    keep, give = split_columns(rank, ref_qkv, policy_key)
    got = swapped(give, "rep", 1)
    other = swapped(tokens, "rep", 1)
    copies = jax.ShapeDtypeStruct((shards, own_features, 7 * HD), bf16)
    pair = jax.ShapeDtypeStruct((2, own_features, width), bf16)
    copies, pair = call(pack, (copies, pair), 0, keep, got)
    column = pair
    for bit in range(1, replicas.bit_length() - 1):
        column = jnp.concatenate([column, swapped(column, "rep", 1 << bit)])
    gathered = exchanged(copies, "fsdp").reshape(features, -1)
    both = jnp.stack([column, swapped(column, "fsdp", length)])
    up, down = [both], [both]
    for k in range(1, length // 2 + 1):
        up.append(passed(up[-1], 1))
        if k < length // 2 or length == 1:
            down.append(passed(down[-1], -1))
    place = jnp.stack([shard % length, shard // length, rank]).astype(jnp.int32)
    whole = arranged(place, up + down[:0:-1]).reshape(-1, width)

    seg = segment_ids[0]
    start = rank * mine
    my_seg = lax.dynamic_slice_in_dim(seg, start, mine, 0)
    before = jnp.sum((seg[None, :] < my_seg[:, None]).astype(jnp.int32), axis=1)
    pos = start + jnp.arange(mine, dtype=jnp.int32) - before
    freq = 1000000.0 ** (-2.0 * jnp.arange(HALF, dtype=f32) / HD)
    angle = pos.astype(f32)[:, None] * freq[None, :]
    cosine, sine = jnp.cos(angle), jnp.sin(angle)
    cosine = jnp.concatenate([cosine, cosine], axis=1)
    sine = jnp.concatenate([-sine, sine], axis=1)
    bias = ref_bias.reshape(SHARE + 2, HD)

    part = projected(tokens, other, gathered, replicas)
    part = exchanged(part, "rep")
    my_kv = call(
        keys_and_values,
        (jax.ShapeDtypeStruct((replicas, 2 * mine, HD), bf16),),
        16 * mine * HD,
        part,
        bias,
        cosine,
        sine,
    )
    all_kv = exchanged(my_kv, "rep")
    window = min(WINDOW, replicas)
    query, mask = call(
        queries,
        (
            jax.ShapeDtypeStruct((SHARE, mine, HD), bf16),
            jax.ShapeDtypeStruct((mine, window * mine), f32),
        ),
        32 * SHARE * mine * HD,
        rank.reshape(1),
        part,
        bias,
        cosine,
        sine,
        seg.reshape(replicas, mine),
        my_seg[:, None],
        scalars=1,
    )
    context = call(
        attend,
        (jax.ShapeDtypeStruct((mine, SHARE * HD), bf16),),
        4 * SHARE * mine * window * mine * HD,
        rank.reshape(1),
        query,
        mask,
        all_kv,
        scalars=1,
    )
    return (context, whole)


def solution(mesh):
    in_specs = (
        P("fsdp", "rep"),
        P(("rep", "fsdp"), "tp"),
        P("tp"),
        P("fsdp", None),
        P(("rep", "fsdp"), "tp"),
    )
    out_specs = (P(("fsdp", "rep"), "tp"), P(None, "tp"))
    return jax.shard_map(body, mesh=mesh, in_specs=in_specs, out_specs=out_specs, check_vma=False)
```

```python
import jax
import jax.numpy as jnp
from jax import lax
from jax.experimental import pallas as pl
from jax.experimental.pallas import tpu as pltpu
from jax.sharding import PartitionSpec as P


QH = 40
KVH = 8
HD = 128
HALF = HD // 2
SHARE = QH // KVH
SIDES = 2
WINDOW = 5


def exchanged(blocks, axis):
    return lax.all_to_all(blocks, axis, split_axis=0, concat_axis=0, tiled=True)


def cost(flops, moved):
    return pl.CostEstimate(flops=flops, bytes_accessed=moved, transcendentals=0)


def call(kernel, outs, flops, *args, scalars=0):
    vmem = pl.BlockSpec(memory_space=pltpu.VMEM)
    smem = pl.BlockSpec(memory_space=pltpu.SMEM)
    moved = sum(a.size * a.dtype.itemsize for a in (*args, *outs))
    return pl.pallas_call(
        kernel,
        out_shape=outs if len(outs) > 1 else outs[0],
        in_specs=[smem] * scalars + [vmem] * (len(args) - scalars),
        out_specs=tuple(vmem for _ in outs) if len(outs) > 1 else vmem,
        compiler_params=pltpu.CompilerParams(vmem_limit_bytes=24 * 1024 * 1024),
        cost_estimate=cost(flops, moved),
    )(*args)


def lanes_below_half(shape):
    return lax.broadcasted_iota(jnp.int32, shape, len(shape) - 1) < HALF


def split(rank_ref, w_hbm, policy_hbm, keep_ref, give_ref, w_ref, policy_ref, sems):
    loads = [
        pltpu.make_async_copy(w_hbm, w_ref, sems.at[0]),
        pltpu.make_async_copy(policy_hbm, policy_ref, sems.at[1]),
    ]
    for load in loads:
        load.start()
    for load in loads:
        load.wait()
    key, val = w_ref[:, 5 * HD : 6 * HD], w_ref[:, 6 * HD :]
    low, high = w_ref[:, : 2 * HD], w_ref[:, 3 * HD : 5 * HD]
    left, right = w_ref[:, 2 * HD : 2 * HD + HALF], w_ref[:, 2 * HD + HALF : 3 * HD]
    odd = jnp.bitwise_and(rank_ref[0], 1)

    @pl.when(odd == 0)
    def _():
        keep_ref[...] = jnp.concatenate([key, low, left, policy_ref[...]], axis=1)
        give_ref[...] = jnp.concatenate([right, val, high, policy_ref[...]], axis=1)

    @pl.when(odd == 1)
    def _():
        keep_ref[...] = jnp.concatenate([val, high, right, policy_ref[...]], axis=1)
        give_ref[...] = jnp.concatenate([left, key, low, policy_ref[...]], axis=1)


def split_columns(rank, w, policy):
    vmem = pl.BlockSpec(memory_space=pltpu.VMEM)
    hbm = pl.BlockSpec(memory_space=pltpu.HBM)
    rows = w.shape[0]
    return pl.pallas_call(
        split,
        out_shape=(jax.ShapeDtypeStruct((rows, 7 * HALF + policy.shape[1]), w.dtype),) * 2,
        in_specs=[pl.BlockSpec(memory_space=pltpu.SMEM), hbm, hbm],
        out_specs=(vmem, vmem),
        scratch_shapes=[
            pltpu.VMEM(w.shape, w.dtype),
            pltpu.VMEM(policy.shape, policy.dtype),
            pltpu.SemaphoreType.DMA((2,)),
        ],
        compiler_params=pltpu.CompilerParams(vmem_limit_bytes=67_000_000),
        cost_estimate=cost(0, 8 * w.size),
    )(rank.reshape(1), w, policy)


def pack(keep_ref, got_ref, out_ref, pair_ref):
    row = jnp.concatenate([keep_ref[:, : 7 * HALF], got_ref[:, : 7 * HALF]], axis=1)
    for j in range(out_ref.shape[0]):
        out_ref[j] = row
    pair_ref[0] = keep_ref[:, 7 * HALF :]
    pair_ref[1] = got_ref[:, 7 * HALF :]


def arrange(place_ref, *refs):
    *parts, out_ref, sem = refs
    x, y, z = place_ref[0], place_ref[1], place_ref[2]
    way = 1 - 2 * jnp.bitwise_and(z, 1)
    length, sides, replicas = len(parts), out_ref.shape[1], out_ref.shape[0]
    copies = []
    for k, part in enumerate(parts):
        distance = k if k <= length // 2 else k - length
        column = jnp.bitwise_and(x - distance, length - 1)
        for side in range(sides):
            for b in range(replicas):
                source = jnp.bitwise_and(z + way * (b - b % 2), replicas - 1) ^ (b % 2)
                place = out_ref.at[source, y ^ side, column]
                copies.append(pltpu.make_async_copy(part.at[side, b], place, sem))
    for copy in copies:
        copy.start()
    pltpu.make_async_copy(out_ref, out_ref, sem).wait()


def arranged(place, parts):
    sides, replicas, rows, width = parts[0].shape
    hbm = pl.BlockSpec(memory_space=pl.ANY)
    return pl.pallas_call(
        arrange,
        out_shape=jax.ShapeDtypeStruct((replicas, sides, len(parts), rows, width), parts[0].dtype),
        in_specs=[pl.BlockSpec(memory_space=pltpu.SMEM)] + [hbm] * len(parts),
        out_specs=hbm,
        scratch_shapes=[pltpu.SemaphoreType.DMA],
        compiler_params=pltpu.CompilerParams(vmem_limit_bytes=1024 * 1024),
        cost_estimate=cost(0, 4 * len(parts) * parts[0].size),
    )(place, *parts)


def project(own_ref, other_ref, w_ref, out_ref):
    blocks = out_ref.shape[0]
    rows = own_ref.shape[0]
    step = rows // 2
    shared = w_ref[:, 3 * HD : 4 * HD]
    w_own = w_ref[:, : 4 * HD]
    swapped = pltpu.roll(shared.astype(jnp.float32), HALF, 1).astype(jnp.bfloat16)
    w_other = jnp.concatenate([w_ref[:, 4 * HD :], swapped], axis=1)
    size = rows // blocks
    low = lanes_below_half((size // 2, HD))
    for part in range(2):
        at = part * step
        value = jnp.dot(own_ref[at : at + step, :], w_own, preferred_element_type=jnp.float32)
        value = value + jnp.dot(
            other_ref[at : at + step, :], w_other, preferred_element_type=jnp.float32
        )
        for b in range(step // size):
            j = at // size + b
            piece = value[b * size : (b + 1) * size]
            for c in range(3):
                out_ref[j, c * size : (c + 1) * size] = piece[:, c * HD : (c + 1) * HD].astype(
                    jnp.bfloat16
                )
            last = piece[:, 3 * HD :]
            packed = jnp.where(low, last[: size // 2], pltpu.roll(last[size // 2 :], HALF, 1))
            out_ref[j, 3 * size :] = packed.astype(jnp.bfloat16)


def turned(value, cosine, sine):
    return value * cosine + pltpu.roll(value, HALF, 1) * sine


def added(ref, parity, rows):
    value = ref[parity, rows].astype(jnp.float32)
    for j in range(parity + 2, ref.shape[0], 2):
        value = value + ref[j, rows].astype(jnp.float32)
    return value


def keys_and_values(part_ref, bias_ref, cos_ref, sin_ref, *rest):
    out_ref = rest[-1]
    size = out_ref.shape[1] // 2
    rows = slice(0, size)
    key = added(part_ref, 0, rows) + bias_ref[SHARE : SHARE + 1]
    key = turned(key, cos_ref[...], sin_ref[...]).astype(jnp.bfloat16)
    val = (added(part_ref, 1, rows) + bias_ref[SHARE + 1 : SHARE + 2]).astype(jnp.bfloat16)
    for j in range(out_ref.shape[0]):
        out_ref[j, :size] = key
        out_ref[j, size:] = val


def first_block(rank, blocks, window):
    return jnp.clip(rank - (window - 1), 0, blocks - window)


def queries(rank_ref, part_ref, bias_ref, cos_ref, sin_ref, seg_ref, mine_ref, out_ref, mask_ref):
    size = out_ref.shape[1]
    blocks = seg_ref.shape[0]
    window = mask_ref.shape[1] // size
    rank = rank_ref[0]
    first = first_block(rank, blocks, window)
    low = lanes_below_half((size // 2, HD))
    left = added(part_ref, 0, slice(3 * size, 7 * size // 2))
    right = added(part_ref, 1, slice(3 * size, 7 * size // 2))
    middle = jnp.concatenate(
        [
            jnp.where(low, left, pltpu.roll(right, HALF, 1)),
            jnp.where(low, pltpu.roll(left, HALF, 1), right),
        ],
        axis=0,
    )
    heads = [
        added(part_ref, 0, slice(size, 2 * size)),
        added(part_ref, 0, slice(2 * size, 3 * size)),
        middle,
        added(part_ref, 1, slice(size, 2 * size)),
        added(part_ref, 1, slice(2 * size, 3 * size)),
    ]
    cosine, sine = cos_ref[...], sin_ref[...]
    for h in range(SHARE):
        query = turned(heads[h] + bias_ref[h : h + 1], cosine, sine)
        out_ref[h] = query.astype(jnp.bfloat16)
    row = rank * size + lax.broadcasted_iota(jnp.int32, (size, size), 0)
    lane = lax.broadcasted_iota(jnp.int32, (size, size), 1)
    for b in range(window):
        seg = seg_ref[pl.ds(first + b, 1), :]
        allowed = (mine_ref[...] == seg) & ((first + b) * size + lane <= row)
        mask_ref[:, b * size : (b + 1) * size] = jnp.where(allowed, 0.0, -1e30)


def attend(rank_ref, q_ref, mask_ref, kv_ref, out_ref):
    size = out_ref.shape[0]
    blocks = kv_ref.shape[0]
    window = mask_ref.shape[1] // size
    first = first_block(rank_ref[0], blocks, window)
    span = kv_ref[pl.ds(first, window)]
    keys = span[:, :size].reshape(window * size, HD)
    vals = span[:, size:].reshape(window * size, HD)
    mask = mask_ref[...]
    for h in range(SHARE):
        scores = lax.dot_general(
            q_ref[h], keys, (((1,), (1,)), ((), ())), preferred_element_type=jnp.float32
        )
        scores = scores * (1.0 / HD**0.5) + mask
        top = jnp.max(scores, axis=-1, keepdims=True)
        expo = jnp.exp(scores - top)
        share = 1.0 / jnp.sum(expo, axis=-1, keepdims=True)
        weights = (expo * share).astype(jnp.bfloat16)
        context = jnp.dot(weights, vals, preferred_element_type=jnp.float32)
        out_ref[:, h * HD : (h + 1) * HD] = context.astype(jnp.bfloat16)


def body(tokens, ref_qkv, ref_bias, segment_ids, policy_key):
    replicas = lax.axis_size("rep")
    shards = lax.axis_size("fsdp")
    rows, features = tokens.shape
    mine = rows // replicas
    rank = lax.axis_index("rep")
    bf16, f32 = jnp.bfloat16, jnp.float32
    length = shards // SIDES
    shard = lax.axis_index("fsdp")

    def swapped(value, axis, bit):
        pairs = [(i, i ^ bit) for i in range(lax.axis_size(axis))]
        return lax.ppermute(value, axis, pairs)

    def passed(value, by):
        pairs = [(i, i // length * length + (i + by) % length) for i in range(shards)]
        return lax.ppermute(value, "fsdp", pairs)

    own_features, width = policy_key.shape
    keep, give = split_columns(rank, ref_qkv, policy_key)
    got = swapped(give, "rep", 1)
    other = swapped(tokens, "rep", 1)
    copies = jax.ShapeDtypeStruct((shards, own_features, 7 * HD), bf16)
    pair = jax.ShapeDtypeStruct((2, own_features, width), bf16)
    copies, pair = call(pack, (copies, pair), 0, keep, got)
    column = pair
    for step in (1 << bit for bit in range(1, replicas.bit_length() - 1)):
        pairs = [((i - step if i % 2 else i + step) % replicas, i) for i in range(replicas)]
        column = jnp.concatenate([column, lax.ppermute(column, "rep", pairs)])
    gathered = exchanged(copies, "fsdp").reshape(features, -1)
    both = jnp.stack([column, swapped(column, "fsdp", length)])
    up, down = [both], [both]
    for k in range(1, length // 2 + 1):
        up.append(passed(up[-1], 1))
        if k < length // 2 or length == 1:
            down.append(passed(down[-1], -1))
    place = jnp.stack([shard % length, shard // length, rank]).astype(jnp.int32)
    whole = arranged(place, up + down[:0:-1]).reshape(-1, width)

    seg = segment_ids[0]
    start = rank * mine
    my_seg = lax.dynamic_slice_in_dim(seg, start, mine, 0)
    before = jnp.sum((seg[None, :] < my_seg[:, None]).astype(jnp.int32), axis=1)
    pos = start + jnp.arange(mine, dtype=jnp.int32) - before
    freq = 1000000.0 ** (-2.0 * jnp.arange(HALF, dtype=f32) / HD)
    angle = pos.astype(f32)[:, None] * freq[None, :]
    cosine, sine = jnp.cos(angle), jnp.sin(angle)
    cosine = jnp.concatenate([cosine, cosine], axis=1)
    sine = jnp.concatenate([-sine, sine], axis=1)
    bias = ref_bias.reshape(SHARE + 2, HD)

    part = jax.ShapeDtypeStruct((replicas, 7 * mine // 2, HD), bf16)
    part = call(project, (part,), 4 * rows * features * 4 * HD, tokens, other, gathered)
    part = exchanged(part, "rep")
    my_kv = call(
        keys_and_values,
        (jax.ShapeDtypeStruct((replicas, 2 * mine, HD), bf16),),
        16 * mine * HD,
        part,
        bias,
        cosine,
        sine,
    )
    all_kv = exchanged(my_kv, "rep")
    window = min(WINDOW, replicas)
    query, mask = call(
        queries,
        (
            jax.ShapeDtypeStruct((SHARE, mine, HD), bf16),
            jax.ShapeDtypeStruct((mine, window * mine), f32),
        ),
        32 * SHARE * mine * HD,
        rank.reshape(1),
        part,
        bias,
        cosine,
        sine,
        seg.reshape(replicas, mine),
        my_seg[:, None],
        scalars=1,
    )
    context = call(
        attend,
        (jax.ShapeDtypeStruct((mine, SHARE * HD), bf16),),
        4 * SHARE * mine * window * mine * HD,
        rank.reshape(1),
        query,
        mask,
        all_kv,
        scalars=1,
    )
    return (context, whole)


def solution(mesh):
    in_specs = (
        P("fsdp", "rep"),
        P(("rep", "fsdp"), "tp"),
        P("tp"),
        P("fsdp", None),
        P(("rep", "fsdp"), "tp"),
    )
    out_specs = (P(("fsdp", "rep"), "tp"), P(None, "tp"))
    return jax.shard_map(body, mesh=mesh, in_specs=in_specs, out_specs=out_specs, check_vma=False)
```

```python
import jax
import jax.numpy as jnp
from jax import lax
from jax.experimental import pallas as pl
from jax.experimental.pallas import tpu as pltpu
from jax.sharding import PartitionSpec as P


QH = 40
KVH = 8
HD = 128
HALF = HD // 2
SHARE = QH // KVH
LENGTH = 8
WINDOW = 5


def exchanged(blocks, axis):
    return lax.all_to_all(blocks, axis, split_axis=0, concat_axis=0, tiled=True)


def in_hbm(array):
    return pltpu.with_memory_space_constraint(array, pltpu.HBM)


def cost(flops, moved):
    return pl.CostEstimate(flops=flops, bytes_accessed=moved, transcendentals=0)


def call(kernel, outs, flops, *args, scalars=0):
    vmem = pl.BlockSpec(memory_space=pltpu.VMEM)
    smem = pl.BlockSpec(memory_space=pltpu.SMEM)
    moved = sum(a.size * a.dtype.itemsize for a in (*args, *outs))
    return pl.pallas_call(
        kernel,
        out_shape=outs if len(outs) > 1 else outs[0],
        in_specs=[smem] * scalars + [vmem] * (len(args) - scalars),
        out_specs=tuple(vmem for _ in outs) if len(outs) > 1 else vmem,
        compiler_params=pltpu.CompilerParams(vmem_limit_bytes=24 * 1024 * 1024),
        cost_estimate=cost(flops, moved),
    )(*args)


def lanes_below_half(shape):
    return lax.broadcasted_iota(jnp.int32, shape, len(shape) - 1) < HALF


def split(rank_ref, w_hbm, policy_hbm, keep_ref, give_ref, w_ref, policy_ref, sems):
    loads = [
        pltpu.make_async_copy(w_hbm, w_ref, sems.at[0]),
        pltpu.make_async_copy(policy_hbm, policy_ref, sems.at[1]),
    ]
    for load in loads:
        load.start()
    for load in loads:
        load.wait()
    key, val = w_ref[:, 5 * HD : 6 * HD], w_ref[:, 6 * HD :]
    low, high = w_ref[:, : 2 * HD], w_ref[:, 3 * HD : 5 * HD]
    left, right = w_ref[:, 2 * HD : 2 * HD + HALF], w_ref[:, 2 * HD + HALF : 3 * HD]
    odd = jnp.bitwise_and(rank_ref[0], 1)

    @pl.when(odd == 0)
    def _():
        keep_ref[...] = jnp.concatenate([key, low, left, policy_ref[...]], axis=1)
        give_ref[...] = jnp.concatenate([right, val, high, policy_ref[...]], axis=1)

    @pl.when(odd == 1)
    def _():
        keep_ref[...] = jnp.concatenate([val, high, right, policy_ref[...]], axis=1)
        give_ref[...] = jnp.concatenate([left, key, low, policy_ref[...]], axis=1)


def split_columns(rank, w, policy):
    vmem = pl.BlockSpec(memory_space=pltpu.VMEM)
    hbm = pl.BlockSpec(memory_space=pltpu.HBM)
    rows = w.shape[0]
    return pl.pallas_call(
        split,
        out_shape=(jax.ShapeDtypeStruct((rows, 7 * HALF + policy.shape[1]), w.dtype),) * 2,
        in_specs=[pl.BlockSpec(memory_space=pltpu.SMEM), hbm, hbm],
        out_specs=(vmem, vmem),
        scratch_shapes=[
            pltpu.VMEM(w.shape, w.dtype),
            pltpu.VMEM(policy.shape, policy.dtype),
            pltpu.SemaphoreType.DMA((2,)),
        ],
        compiler_params=pltpu.CompilerParams(vmem_limit_bytes=4 * 1024 * 1024),
        cost_estimate=cost(0, 8 * w.size),
    )(rank.reshape(1), w, policy)


def pack(keep_ref, got_ref, out_ref, pair_ref):
    row = jnp.concatenate([keep_ref[:, : 7 * HALF], got_ref[:, : 7 * HALF]], axis=1)
    for j in range(out_ref.shape[0]):
        out_ref[j] = row
    pair_ref[0] = keep_ref[:, 7 * HALF :]
    pair_ref[1] = got_ref[:, 7 * HALF :]


def arrange(place_ref, own_ref, up_ref, across_ref, down_ref, ups_ref, downs_ref, out_ref, sem):
    x, y, z = place_ref[0], place_ref[1], place_ref[2]
    way = 1 - 2 * jnp.bitwise_and(z, 1)
    replicas, sides, length = out_ref.shape[:3]
    parts = [
        (own_ref, 0),
        (up_ref, 1),
        (ups_ref.at[0], 2),
        (ups_ref.at[1], 3),
        (across_ref, 4),
        (downs_ref.at[1], 5),
        (downs_ref.at[0], 6),
        (down_ref, 7),
    ]
    for part, distance in parts:
        column = jnp.bitwise_and(x - distance, length - 1)
        for side in range(sides):
            for b in range(replicas):
                source = jnp.bitwise_and(z + way * (b - b % 2), replicas - 1) ^ (b % 2)
                place = out_ref.at[source, y ^ side, column]
                pltpu.make_async_copy(part.at[side, b], place, sem).start()
    pltpu.make_async_copy(out_ref, out_ref, sem).wait()


def arranged(place, parts):
    sides, replicas, rows, width = parts[0].shape
    hbm = pl.BlockSpec(memory_space=pl.ANY)
    return pl.pallas_call(
        arrange,
        out_shape=jax.ShapeDtypeStruct((replicas, sides, LENGTH, rows, width), parts[0].dtype),
        in_specs=[pl.BlockSpec(memory_space=pltpu.SMEM)] + [hbm] * len(parts),
        out_specs=hbm,
        scratch_shapes=[pltpu.SemaphoreType.DMA],
        compiler_params=pltpu.CompilerParams(vmem_limit_bytes=1024 * 1024),
        cost_estimate=cost(0, 4 * LENGTH * parts[0].size),
    )(place, *parts)


def project(own_ref, other_ref, w_ref, out_ref):
    blocks = out_ref.shape[0]
    rows = own_ref.shape[0]
    step = rows // 2
    shared = w_ref[:, 3 * HD : 4 * HD]
    w_own = w_ref[:, : 4 * HD]
    swapped = pltpu.roll(shared.astype(jnp.float32), HALF, 1).astype(jnp.bfloat16)
    w_other = jnp.concatenate([w_ref[:, 4 * HD :], swapped], axis=1)
    size = rows // blocks
    low = lanes_below_half((size // 2, HD))
    for part in range(2):
        at = part * step
        value = jnp.dot(own_ref[at : at + step, :], w_own, preferred_element_type=jnp.float32)
        value = value + jnp.dot(
            other_ref[at : at + step, :], w_other, preferred_element_type=jnp.float32
        )
        for b in range(step // size):
            j = at // size + b
            piece = value[b * size : (b + 1) * size]
            for c in range(3):
                out_ref[j, c * size : (c + 1) * size] = piece[:, c * HD : (c + 1) * HD].astype(
                    jnp.bfloat16
                )
            last = piece[:, 3 * HD :]
            packed = jnp.where(low, last[: size // 2], pltpu.roll(last[size // 2 :], HALF, 1))
            out_ref[j, 3 * size :] = packed.astype(jnp.bfloat16)


def turned(value, cosine, sine):
    return value * cosine + pltpu.roll(value, HALF, 1) * sine


def added(ref, parity, rows):
    value = ref[parity, rows].astype(jnp.float32)
    for j in range(parity + 2, ref.shape[0], 2):
        value = value + ref[j, rows].astype(jnp.float32)
    return value


def keys_and_values(part_ref, bias_ref, cos_ref, sin_ref, *rest):
    out_ref = rest[-1]
    size = out_ref.shape[1] // 2
    rows = slice(0, size)
    key = added(part_ref, 0, rows) + bias_ref[SHARE : SHARE + 1]
    key = turned(key, cos_ref[...], sin_ref[...]).astype(jnp.bfloat16)
    val = (added(part_ref, 1, rows) + bias_ref[SHARE + 1 : SHARE + 2]).astype(jnp.bfloat16)
    for j in range(out_ref.shape[0]):
        out_ref[j, :size] = key
        out_ref[j, size:] = val


def first_block(rank, blocks, window):
    return jnp.clip(rank - (window - 1), 0, blocks - window)


def queries(rank_ref, part_ref, bias_ref, cos_ref, sin_ref, seg_ref, mine_ref, out_ref, mask_ref):
    size = out_ref.shape[1]
    blocks = seg_ref.shape[0]
    window = mask_ref.shape[1] // size
    rank = rank_ref[0]
    first = first_block(rank, blocks, window)
    low = lanes_below_half((size // 2, HD))
    left = added(part_ref, 0, slice(3 * size, 7 * size // 2))
    right = added(part_ref, 1, slice(3 * size, 7 * size // 2))
    middle = jnp.concatenate(
        [
            jnp.where(low, left, pltpu.roll(right, HALF, 1)),
            jnp.where(low, pltpu.roll(left, HALF, 1), right),
        ],
        axis=0,
    )
    heads = [
        added(part_ref, 0, slice(size, 2 * size)),
        added(part_ref, 0, slice(2 * size, 3 * size)),
        middle,
        added(part_ref, 1, slice(size, 2 * size)),
        added(part_ref, 1, slice(2 * size, 3 * size)),
    ]
    cosine, sine = cos_ref[...], sin_ref[...]
    for h in range(SHARE):
        query = turned(heads[h] + bias_ref[h : h + 1], cosine, sine)
        out_ref[h] = query.astype(jnp.bfloat16)
    row = rank * size + lax.broadcasted_iota(jnp.int32, (size, size), 0)
    lane = lax.broadcasted_iota(jnp.int32, (size, size), 1)
    for b in range(window):
        seg = seg_ref[pl.ds(first + b, 1), :]
        allowed = (mine_ref[...] == seg) & ((first + b) * size + lane <= row)
        mask_ref[:, b * size : (b + 1) * size] = jnp.where(allowed, 0.0, -1e30)


def attend(rank_ref, q_ref, mask_ref, kv_ref, out_ref):
    size = out_ref.shape[0]
    blocks = kv_ref.shape[0]
    window = mask_ref.shape[1] // size
    first = first_block(rank_ref[0], blocks, window)
    span = kv_ref[pl.ds(first, window)]
    keys = span[:, :size].reshape(window * size, HD)
    vals = span[:, size:].reshape(window * size, HD)
    mask = mask_ref[...]
    for h in range(SHARE):
        scores = lax.dot_general(
            q_ref[h], keys, (((1,), (1,)), ((), ())), preferred_element_type=jnp.float32
        )
        scores = scores * (1.0 / HD**0.5) + mask
        top = jnp.max(scores, axis=-1, keepdims=True)
        expo = jnp.exp(scores - top)
        share = 1.0 / jnp.sum(expo, axis=-1, keepdims=True)
        weights = (expo * share).astype(jnp.bfloat16)
        context = jnp.dot(weights, vals, preferred_element_type=jnp.float32)
        out_ref[:, h * HD : (h + 1) * HD] = context.astype(jnp.bfloat16)


def body(tokens, ref_qkv, ref_bias, segment_ids, policy_key):
    replicas = lax.axis_size("rep")
    shards = lax.axis_size("fsdp")
    rows, features = tokens.shape
    mine = rows // replicas
    rank = lax.axis_index("rep")
    bf16, f32 = jnp.bfloat16, jnp.float32
    length = LENGTH
    shard = lax.axis_index("fsdp")

    def swapped(value, axis, bit):
        pairs = [(i, i ^ bit) for i in range(lax.axis_size(axis))]
        return lax.ppermute(value, axis, pairs)

    def passed(value, by):
        pairs = [(i, i // length * length + (i + by) % length) for i in range(shards)]
        return lax.ppermute(value, "fsdp", pairs)

    own_features, width = policy_key.shape
    keep, give = split_columns(rank, in_hbm(ref_qkv), in_hbm(policy_key))
    got = swapped(give, "rep", 1)
    other = swapped(tokens, "rep", 1)
    copies = jax.ShapeDtypeStruct((shards, own_features, 7 * HD), bf16)
    pair = jax.ShapeDtypeStruct((2, own_features, width), bf16)
    copies, pair = call(pack, (copies, pair), 0, keep, got)
    column = pair
    for step in (1 << bit for bit in range(1, replicas.bit_length() - 1)):
        pairs = [((i - step if i % 2 else i + step) % replicas, i) for i in range(replicas)]
        column = jnp.concatenate([column, lax.ppermute(column, "rep", pairs)])
    gathered = exchanged(copies, "fsdp").reshape(features, -1)
    both = jnp.stack([column, swapped(column, "fsdp", length)])
    up, down = passed(both, 1), passed(both, -1)
    across = passed(both, length // 2)
    ups = passed(jnp.stack([both, up]), 2)
    downs = passed(jnp.stack([both, down]), -2)
    place = jnp.stack([shard % length, shard // length, rank]).astype(jnp.int32)
    whole = arranged(place, [both, up, across, down, ups, downs]).reshape(-1, width)

    seg = segment_ids[0]
    start = rank * mine
    my_seg = lax.dynamic_slice_in_dim(seg, start, mine, 0)
    before = jnp.sum((seg[None, :] < my_seg[:, None]).astype(jnp.int32), axis=1)
    pos = start + jnp.arange(mine, dtype=jnp.int32) - before
    freq = 1000000.0 ** (-2.0 * jnp.arange(HALF, dtype=f32) / HD)
    angle = pos.astype(f32)[:, None] * freq[None, :]
    cosine, sine = jnp.cos(angle), jnp.sin(angle)
    cosine = jnp.concatenate([cosine, cosine], axis=1)
    sine = jnp.concatenate([-sine, sine], axis=1)
    bias = ref_bias.reshape(SHARE + 2, HD)

    part = jax.ShapeDtypeStruct((replicas, 7 * mine // 2, HD), bf16)
    part = call(project, (part,), 4 * rows * features * 4 * HD, tokens, other, in_hbm(gathered))
    part = exchanged(part, "rep")
    my_kv = call(
        keys_and_values,
        (jax.ShapeDtypeStruct((replicas, 2 * mine, HD), bf16),),
        16 * mine * HD,
        part,
        bias,
        cosine,
        sine,
    )
    all_kv = exchanged(my_kv, "rep")
    window = min(WINDOW, replicas)
    query, mask = call(
        queries,
        (
            jax.ShapeDtypeStruct((SHARE, mine, HD), bf16),
            jax.ShapeDtypeStruct((mine, window * mine), f32),
        ),
        32 * SHARE * mine * HD,
        rank.reshape(1),
        part,
        bias,
        cosine,
        sine,
        seg.reshape(replicas, mine),
        my_seg[:, None],
        scalars=1,
    )
    context = call(
        attend,
        (jax.ShapeDtypeStruct((mine, SHARE * HD), bf16),),
        4 * SHARE * mine * window * mine * HD,
        rank.reshape(1),
        query,
        mask,
        all_kv,
        scalars=1,
    )
    return (context, whole)


def solution(mesh):
    in_specs = (
        P("fsdp", "rep"),
        P(("rep", "fsdp"), "tp"),
        P("tp"),
        P("fsdp", None),
        P(("rep", "fsdp"), "tp"),
    )
    out_specs = (P(("fsdp", "rep"), "tp"), P(None, "tp"))
    return jax.shard_map(body, mesh=mesh, in_specs=in_specs, out_specs=out_specs, check_vma=False)
```

```python
import jax
import jax.numpy as jnp
from jax import lax
from jax.experimental import pallas as pl
from jax.experimental.pallas import tpu as pltpu
from jax.sharding import PartitionSpec as P


QH = 40
KVH = 8
HD = 128
HALF = HD // 2
SHARE = QH // KVH
SIDES = 2
WINDOW = 5


def exchanged(blocks, axis):
    return lax.all_to_all(blocks, axis, split_axis=0, concat_axis=0, tiled=True)


def in_hbm(array):
    return pltpu.with_memory_space_constraint(array, pltpu.HBM)


def cost(flops, moved):
    return pl.CostEstimate(flops=flops, bytes_accessed=moved, transcendentals=0)


def call(kernel, outs, flops, *args, scalars=0):
    vmem = pl.BlockSpec(memory_space=pltpu.VMEM)
    smem = pl.BlockSpec(memory_space=pltpu.SMEM)
    moved = sum(a.size * a.dtype.itemsize for a in (*args, *outs))
    return pl.pallas_call(
        kernel,
        out_shape=outs if len(outs) > 1 else outs[0],
        in_specs=[smem] * scalars + [vmem] * (len(args) - scalars),
        out_specs=tuple(vmem for _ in outs) if len(outs) > 1 else vmem,
        compiler_params=pltpu.CompilerParams(vmem_limit_bytes=24 * 1024 * 1024),
        cost_estimate=cost(flops, moved),
    )(*args)


def lanes_below_half(shape):
    return lax.broadcasted_iota(jnp.int32, shape, len(shape) - 1) < HALF


def split(rank_ref, w_hbm, policy_hbm, keep_ref, give_ref, w_ref, policy_ref, sems):
    loads = [
        pltpu.make_async_copy(w_hbm, w_ref, sems.at[0]),
        pltpu.make_async_copy(policy_hbm, policy_ref, sems.at[1]),
    ]
    for load in loads:
        load.start()
    for load in loads:
        load.wait()
    key, val = w_ref[:, 5 * HD : 6 * HD], w_ref[:, 6 * HD :]
    low, high = w_ref[:, : 2 * HD], w_ref[:, 3 * HD : 5 * HD]
    left, right = w_ref[:, 2 * HD : 2 * HD + HALF], w_ref[:, 2 * HD + HALF : 3 * HD]
    odd = jnp.bitwise_and(rank_ref[0], 1)

    @pl.when(odd == 0)
    def _():
        keep_ref[...] = jnp.concatenate([key, low, left, policy_ref[...]], axis=1)
        give_ref[...] = jnp.concatenate([right, val, high, policy_ref[...]], axis=1)

    @pl.when(odd == 1)
    def _():
        keep_ref[...] = jnp.concatenate([val, high, right, policy_ref[...]], axis=1)
        give_ref[...] = jnp.concatenate([left, key, low, policy_ref[...]], axis=1)


def split_columns(rank, w, policy):
    vmem = pl.BlockSpec(memory_space=pltpu.VMEM)
    hbm = pl.BlockSpec(memory_space=pltpu.HBM)
    rows = w.shape[0]
    return pl.pallas_call(
        split,
        out_shape=(jax.ShapeDtypeStruct((rows, 7 * HALF + policy.shape[1]), w.dtype),) * 2,
        in_specs=[pl.BlockSpec(memory_space=pltpu.SMEM), hbm, hbm],
        out_specs=(vmem, vmem),
        scratch_shapes=[
            pltpu.VMEM(w.shape, w.dtype),
            pltpu.VMEM(policy.shape, policy.dtype),
            pltpu.SemaphoreType.DMA((2,)),
        ],
        compiler_params=pltpu.CompilerParams(vmem_limit_bytes=4 * 1024 * 1024),
        cost_estimate=cost(0, 8 * w.size),
    )(rank.reshape(1), w, policy)


def pack(keep_ref, got_ref, out_ref, pair_ref):
    row = jnp.concatenate([keep_ref[:, : 7 * HALF], got_ref[:, : 7 * HALF]], axis=1)
    for j in range(out_ref.shape[0]):
        out_ref[j] = row
    pair_ref[0] = keep_ref[:, 7 * HALF :]
    pair_ref[1] = got_ref[:, 7 * HALF :]


def arrange(place_ref, *refs):
    *parts, out_ref, sem = refs
    x, y, z = place_ref[0], place_ref[1], place_ref[2]
    way = 1 - 2 * jnp.bitwise_and(z, 1)
    length, sides, replicas = len(parts), out_ref.shape[1], out_ref.shape[0]
    copies = []
    for k, part in enumerate(parts):
        distance = k if k <= length // 2 else k - length
        column = jnp.bitwise_and(x - distance, length - 1)
        for side in range(sides):
            for b in range(replicas):
                source = jnp.bitwise_and(z + way * (b - b % 2), replicas - 1) ^ (b % 2)
                place = out_ref.at[source, y ^ side, column]
                copies.append(pltpu.make_async_copy(part.at[side, b], place, sem))
    for copy in copies:
        copy.start()
    pltpu.make_async_copy(out_ref, out_ref, sem).wait()


def arranged(place, parts):
    sides, replicas, rows, width = parts[0].shape
    hbm = pl.BlockSpec(memory_space=pl.ANY)
    return pl.pallas_call(
        arrange,
        out_shape=jax.ShapeDtypeStruct((replicas, sides, len(parts), rows, width), parts[0].dtype),
        in_specs=[pl.BlockSpec(memory_space=pltpu.SMEM)] + [hbm] * len(parts),
        out_specs=hbm,
        scratch_shapes=[pltpu.SemaphoreType.DMA],
        compiler_params=pltpu.CompilerParams(vmem_limit_bytes=1024 * 1024),
        cost_estimate=cost(0, 4 * len(parts) * parts[0].size),
    )(place, *parts)


def project(own_hbm, other_hbm, w_ref, out_ref, own_ref, other_ref, sems):
    blocks = out_ref.shape[0]
    rows = own_hbm.shape[0]
    step = rows // 2
    loads = []
    for part in range(2):
        span = pl.ds(part * step, step)
        for side, (source, target) in enumerate([(own_hbm, own_ref), (other_hbm, other_ref)]):
            loads.append(
                pltpu.make_async_copy(source.at[span], target.at[span], sems.at[2 * part + side])
            )
    for load in loads:
        load.start()
    shared = w_ref[:, 3 * HD : 4 * HD]
    w_own = w_ref[:, : 4 * HD]
    swapped = pltpu.roll(shared.astype(jnp.float32), HALF, 1).astype(jnp.bfloat16)
    w_other = jnp.concatenate([w_ref[:, 4 * HD :], swapped], axis=1)
    size = rows // blocks
    low = lanes_below_half((size // 2, HD))
    for part in range(2):
        at = part * step
        loads[2 * part].wait()
        loads[2 * part + 1].wait()
        value = jnp.dot(own_ref[at : at + step, :], w_own, preferred_element_type=jnp.float32)
        value = value + jnp.dot(
            other_ref[at : at + step, :], w_other, preferred_element_type=jnp.float32
        )
        for b in range(step // size):
            j = at // size + b
            piece = value[b * size : (b + 1) * size]
            for c in range(3):
                out_ref[j, c * size : (c + 1) * size] = piece[:, c * HD : (c + 1) * HD].astype(
                    jnp.bfloat16
                )
            last = piece[:, 3 * HD :]
            packed = jnp.where(low, last[: size // 2], pltpu.roll(last[size // 2 :], HALF, 1))
            out_ref[j, 3 * size :] = packed.astype(jnp.bfloat16)


def projected(own, other, gathered, blocks):
    rows, features = own.shape
    vmem = pl.BlockSpec(memory_space=pltpu.VMEM)
    hbm = pl.BlockSpec(memory_space=pltpu.HBM)
    return pl.pallas_call(
        project,
        out_shape=jax.ShapeDtypeStruct((blocks, 7 * rows // blocks // 2, HD), jnp.bfloat16),
        in_specs=[hbm, hbm, vmem],
        out_specs=vmem,
        scratch_shapes=[
            pltpu.VMEM(own.shape, own.dtype),
            pltpu.VMEM(own.shape, own.dtype),
            pltpu.SemaphoreType.DMA((4,)),
        ],
        compiler_params=pltpu.CompilerParams(vmem_limit_bytes=24 * 1024 * 1024),
        cost_estimate=cost(4 * rows * features * 4 * HD, 4 * own.size + 2 * gathered.size),
    )(in_hbm(own), in_hbm(other), gathered)


def turned(value, cosine, sine):
    return value * cosine + pltpu.roll(value, HALF, 1) * sine


def added(ref, parity, rows):
    value = ref[parity, rows].astype(jnp.float32)
    for j in range(parity + 2, ref.shape[0], 2):
        value = value + ref[j, rows].astype(jnp.float32)
    return value


def keys_and_values(part_ref, bias_ref, cos_ref, sin_ref, *rest):
    out_ref = rest[-1]
    size = out_ref.shape[1] // 2
    rows = slice(0, size)
    key = added(part_ref, 0, rows) + bias_ref[SHARE : SHARE + 1]
    key = turned(key, cos_ref[...], sin_ref[...]).astype(jnp.bfloat16)
    val = (added(part_ref, 1, rows) + bias_ref[SHARE + 1 : SHARE + 2]).astype(jnp.bfloat16)
    for j in range(out_ref.shape[0]):
        out_ref[j, :size] = key
        out_ref[j, size:] = val


def first_block(rank, blocks, window):
    return jnp.clip(rank - (window - 1), 0, blocks - window)


def queries(rank_ref, part_ref, bias_ref, cos_ref, sin_ref, seg_ref, mine_ref, out_ref, mask_ref):
    size = out_ref.shape[1]
    blocks = seg_ref.shape[0]
    window = mask_ref.shape[1] // size
    rank = rank_ref[0]
    first = first_block(rank, blocks, window)
    low = lanes_below_half((size // 2, HD))
    left = added(part_ref, 0, slice(3 * size, 7 * size // 2))
    right = added(part_ref, 1, slice(3 * size, 7 * size // 2))
    middle = jnp.concatenate(
        [
            jnp.where(low, left, pltpu.roll(right, HALF, 1)),
            jnp.where(low, pltpu.roll(left, HALF, 1), right),
        ],
        axis=0,
    )
    heads = [
        added(part_ref, 0, slice(size, 2 * size)),
        added(part_ref, 0, slice(2 * size, 3 * size)),
        middle,
        added(part_ref, 1, slice(size, 2 * size)),
        added(part_ref, 1, slice(2 * size, 3 * size)),
    ]
    cosine, sine = cos_ref[...], sin_ref[...]
    for h in range(SHARE):
        query = turned(heads[h] + bias_ref[h : h + 1], cosine, sine)
        out_ref[h] = query.astype(jnp.bfloat16)
    row = rank * size + lax.broadcasted_iota(jnp.int32, (size, size), 0)
    lane = lax.broadcasted_iota(jnp.int32, (size, size), 1)
    for b in range(window):
        seg = seg_ref[pl.ds(first + b, 1), :]
        allowed = (mine_ref[...] == seg) & ((first + b) * size + lane <= row)
        mask_ref[:, b * size : (b + 1) * size] = jnp.where(allowed, 0.0, -1e30)


def attend(rank_ref, q_ref, mask_ref, kv_ref, out_ref):
    size = out_ref.shape[0]
    blocks = kv_ref.shape[0]
    window = mask_ref.shape[1] // size
    first = first_block(rank_ref[0], blocks, window)
    span = kv_ref[pl.ds(first, window)]
    keys = span[:, :size].reshape(window * size, HD)
    vals = span[:, size:].reshape(window * size, HD)
    mask = mask_ref[...]
    for h in range(SHARE):
        scores = lax.dot_general(
            q_ref[h], keys, (((1,), (1,)), ((), ())), preferred_element_type=jnp.float32
        )
        scores = scores * (1.0 / HD**0.5) + mask
        top = jnp.max(scores, axis=-1, keepdims=True)
        expo = jnp.exp(scores - top)
        share = 1.0 / jnp.sum(expo, axis=-1, keepdims=True)
        weights = (expo * share).astype(jnp.bfloat16)
        context = jnp.dot(weights, vals, preferred_element_type=jnp.float32)
        out_ref[:, h * HD : (h + 1) * HD] = context.astype(jnp.bfloat16)


def body(tokens, ref_qkv, ref_bias, segment_ids, policy_key):
    replicas = lax.axis_size("rep")
    shards = lax.axis_size("fsdp")
    rows, features = tokens.shape
    mine = rows // replicas
    rank = lax.axis_index("rep")
    bf16, f32 = jnp.bfloat16, jnp.float32
    length = shards // SIDES
    shard = lax.axis_index("fsdp")

    def swapped(value, axis, bit):
        pairs = [(i, i ^ bit) for i in range(lax.axis_size(axis))]
        return lax.ppermute(value, axis, pairs)

    def passed(value, by):
        pairs = [(i, i // length * length + (i + by) % length) for i in range(shards)]
        return lax.ppermute(value, "fsdp", pairs)

    own_features, width = policy_key.shape
    keep, give = split_columns(rank, in_hbm(ref_qkv), in_hbm(policy_key))
    got = swapped(give, "rep", 1)
    other = swapped(tokens, "rep", 1)
    copies = jax.ShapeDtypeStruct((shards, own_features, 7 * HD), bf16)
    pair = jax.ShapeDtypeStruct((2, own_features, width), bf16)
    copies, pair = call(pack, (copies, pair), 0, keep, got)
    column = pair
    for step in (1 << bit for bit in range(1, replicas.bit_length() - 1)):
        pairs = [((i - step if i % 2 else i + step) % replicas, i) for i in range(replicas)]
        column = jnp.concatenate([column, lax.ppermute(column, "rep", pairs)])
    gathered = exchanged(copies, "fsdp").reshape(features, -1)
    both = jnp.stack([column, swapped(column, "fsdp", length)])
    up, down = [both], [both]
    for k in range(1, length // 2 + 1):
        up.append(passed(up[-1], 1))
        if k < length // 2 or length == 1:
            down.append(passed(down[-1], -1))
    place = jnp.stack([shard % length, shard // length, rank]).astype(jnp.int32)
    whole = arranged(place, up + down[:0:-1]).reshape(-1, width)

    seg = segment_ids[0]
    start = rank * mine
    my_seg = lax.dynamic_slice_in_dim(seg, start, mine, 0)
    before = jnp.sum((seg[None, :] < my_seg[:, None]).astype(jnp.int32), axis=1)
    pos = start + jnp.arange(mine, dtype=jnp.int32) - before
    freq = 1000000.0 ** (-2.0 * jnp.arange(HALF, dtype=f32) / HD)
    angle = pos.astype(f32)[:, None] * freq[None, :]
    cosine, sine = jnp.cos(angle), jnp.sin(angle)
    cosine = jnp.concatenate([cosine, cosine], axis=1)
    sine = jnp.concatenate([-sine, sine], axis=1)
    bias = ref_bias.reshape(SHARE + 2, HD)

    part = projected(tokens, other, gathered, replicas)
    part = exchanged(part, "rep")
    my_kv = call(
        keys_and_values,
        (jax.ShapeDtypeStruct((replicas, 2 * mine, HD), bf16),),
        16 * mine * HD,
        part,
        bias,
        cosine,
        sine,
    )
    all_kv = exchanged(my_kv, "rep")
    window = min(WINDOW, replicas)
    query, mask = call(
        queries,
        (
            jax.ShapeDtypeStruct((SHARE, mine, HD), bf16),
            jax.ShapeDtypeStruct((mine, window * mine), f32),
        ),
        32 * SHARE * mine * HD,
        rank.reshape(1),
        part,
        bias,
        cosine,
        sine,
        seg.reshape(replicas, mine),
        my_seg[:, None],
        scalars=1,
    )
    context = call(
        attend,
        (jax.ShapeDtypeStruct((mine, SHARE * HD), bf16),),
        4 * SHARE * mine * window * mine * HD,
        rank.reshape(1),
        query,
        mask,
        all_kv,
        scalars=1,
    )
    return (context, whole)


def solution(mesh):
    in_specs = (
        P("fsdp", "rep"),
        P(("rep", "fsdp"), "tp"),
        P("tp"),
        P("fsdp", None),
        P(("rep", "fsdp"), "tp"),
    )
    out_specs = (P(("fsdp", "rep"), "tp"), P(None, "tp"))
    return jax.shard_map(body, mesh=mesh, in_specs=in_specs, out_specs=out_specs, check_vma=False)
```

```python
import jax
import jax.numpy as jnp
from jax import lax
from jax.experimental import pallas as pl
from jax.experimental.pallas import tpu as pltpu
from jax.sharding import PartitionSpec as P


QH = 40
KVH = 8
HD = 128
HALF = HD // 2
SHARE = QH // KVH
SIDES = 2
WINDOW = 5


def exchanged(blocks, axis):
    return lax.all_to_all(blocks, axis, split_axis=0, concat_axis=0, tiled=True)


def in_hbm(array):
    return pltpu.with_memory_space_constraint(array, pltpu.HBM)


def cost(flops, moved):
    return pl.CostEstimate(flops=flops, bytes_accessed=moved, transcendentals=0)


def call(kernel, outs, flops, *args, scalars=0):
    vmem = pl.BlockSpec(memory_space=pltpu.VMEM)
    smem = pl.BlockSpec(memory_space=pltpu.SMEM)
    moved = sum(a.size * a.dtype.itemsize for a in (*args, *outs))
    return pl.pallas_call(
        kernel,
        out_shape=outs if len(outs) > 1 else outs[0],
        in_specs=[smem] * scalars + [vmem] * (len(args) - scalars),
        out_specs=tuple(vmem for _ in outs) if len(outs) > 1 else vmem,
        compiler_params=pltpu.CompilerParams(vmem_limit_bytes=24 * 1024 * 1024),
        cost_estimate=cost(flops, moved),
    )(*args)


def lanes_below_half(shape):
    return lax.broadcasted_iota(jnp.int32, shape, len(shape) - 1) < HALF


def split(rank_ref, w_hbm, policy_hbm, keep_ref, give_ref, w_ref, policy_ref, sems):
    loads = [
        pltpu.make_async_copy(w_hbm, w_ref, sems.at[0]),
        pltpu.make_async_copy(policy_hbm, policy_ref, sems.at[1]),
    ]
    for load in loads:
        load.start()
    for load in loads:
        load.wait()
    key, val = w_ref[:, 5 * HD : 6 * HD], w_ref[:, 6 * HD :]
    low, high = w_ref[:, : 2 * HD], w_ref[:, 3 * HD : 5 * HD]
    left, right = w_ref[:, 2 * HD : 2 * HD + HALF], w_ref[:, 2 * HD + HALF : 3 * HD]
    odd = jnp.bitwise_and(rank_ref[0], 1)

    @pl.when(odd == 0)
    def _():
        keep_ref[...] = jnp.concatenate([key, low, left, policy_ref[...]], axis=1)
        give_ref[...] = jnp.concatenate([right, val, high, policy_ref[...]], axis=1)

    @pl.when(odd == 1)
    def _():
        keep_ref[...] = jnp.concatenate([val, high, right, policy_ref[...]], axis=1)
        give_ref[...] = jnp.concatenate([left, key, low, policy_ref[...]], axis=1)


def split_columns(rank, w, policy):
    vmem = pl.BlockSpec(memory_space=pltpu.VMEM)
    hbm = pl.BlockSpec(memory_space=pltpu.HBM)
    rows = w.shape[0]
    return pl.pallas_call(
        split,
        out_shape=(jax.ShapeDtypeStruct((rows, 7 * HALF + policy.shape[1]), w.dtype),) * 2,
        in_specs=[pl.BlockSpec(memory_space=pltpu.SMEM), hbm, hbm],
        out_specs=(vmem, vmem),
        scratch_shapes=[
            pltpu.VMEM(w.shape, w.dtype),
            pltpu.VMEM(policy.shape, policy.dtype),
            pltpu.SemaphoreType.DMA((2,)),
        ],
        compiler_params=pltpu.CompilerParams(vmem_limit_bytes=4 * 1024 * 1024),
        cost_estimate=cost(0, 8 * w.size),
    )(rank.reshape(1), w, policy)


def pack(keep_ref, got_ref, out_ref, pair_ref):
    row = jnp.concatenate([keep_ref[:, : 7 * HALF], got_ref[:, : 7 * HALF]], axis=1)
    for j in range(out_ref.shape[0]):
        out_ref[j] = row
    pair_ref[0] = keep_ref[:, 7 * HALF :]
    pair_ref[1] = got_ref[:, 7 * HALF :]


def arrange(place_ref, *refs):
    *parts, out_ref, sem = refs
    x, y, z = place_ref[0], place_ref[1], place_ref[2]
    way = 1 - 2 * jnp.bitwise_and(z, 1)
    length, sides, replicas = len(parts), out_ref.shape[1], out_ref.shape[0]
    copies = []
    for k, part in enumerate(parts):
        distance = k if k <= length // 2 else k - length
        column = jnp.bitwise_and(x - distance, length - 1)
        for side in range(sides):
            for b in range(replicas):
                source = jnp.bitwise_and(z + way * (b - b % 2), replicas - 1) ^ (b % 2)
                place = out_ref.at[source, y ^ side, column]
                copies.append(pltpu.make_async_copy(part.at[side, b], place, sem))
    for copy in copies:
        copy.start()
    pltpu.make_async_copy(out_ref, out_ref, sem).wait()


def arranged(place, parts):
    sides, replicas, rows, width = parts[0].shape
    hbm = pl.BlockSpec(memory_space=pl.ANY)
    return pl.pallas_call(
        arrange,
        out_shape=jax.ShapeDtypeStruct((replicas, sides, len(parts), rows, width), parts[0].dtype),
        in_specs=[pl.BlockSpec(memory_space=pltpu.SMEM)] + [hbm] * len(parts),
        out_specs=hbm,
        scratch_shapes=[pltpu.SemaphoreType.DMA],
        compiler_params=pltpu.CompilerParams(vmem_limit_bytes=1024 * 1024),
        cost_estimate=cost(0, 4 * len(parts) * parts[0].size),
    )(place, *parts)


def project(core_ref, own_hbm, far_hbm, near_hbm, w_ref, out_ref, own_ref, other_ref, sems):
    blocks = out_ref.shape[0]
    rows = own_hbm.shape[0]
    step = rows // 2
    core = core_ref[0]
    loads = []
    for part in range(2):
        span = pl.ds(part * step, step)
        loads.append(pltpu.make_async_copy(own_hbm.at[span], own_ref.at[span], sems.at[part]))
    for source, index in ((far_hbm, core), (near_hbm, 1 - core)):
        span = pl.ds(pl.multiple_of(index * step, step), step)
        loads.append(pltpu.make_async_copy(source, other_ref.at[span], sems.at[len(loads)]))
    for load in loads:
        load.start()
    shared = w_ref[:, 3 * HD : 4 * HD]
    w_own = w_ref[:, : 4 * HD]
    swapped = pltpu.roll(shared.astype(jnp.float32), HALF, 1).astype(jnp.bfloat16)
    w_other = jnp.concatenate([w_ref[:, 4 * HD :], swapped], axis=1)
    size = rows // blocks
    low = lanes_below_half((size // 2, HD))
    for part in range(2):
        at = part * step
        loads[part].wait()
        if part == 0:
            loads[2].wait()
            loads[3].wait()
        value = jnp.dot(own_ref[at : at + step, :], w_own, preferred_element_type=jnp.float32)
        value = value + jnp.dot(
            other_ref[at : at + step, :], w_other, preferred_element_type=jnp.float32
        )
        for b in range(step // size):
            j = at // size + b
            piece = value[b * size : (b + 1) * size]
            for c in range(3):
                out_ref[j, c * size : (c + 1) * size] = piece[:, c * HD : (c + 1) * HD].astype(
                    jnp.bfloat16
                )
            last = piece[:, 3 * HD :]
            packed = jnp.where(low, last[: size // 2], pltpu.roll(last[size // 2 :], HALF, 1))
            out_ref[j, 3 * size :] = packed.astype(jnp.bfloat16)


def projected(core, own, far, near, gathered, blocks):
    rows, features = own.shape
    vmem = pl.BlockSpec(memory_space=pltpu.VMEM)
    hbm = pl.BlockSpec(memory_space=pltpu.HBM)
    return pl.pallas_call(
        project,
        out_shape=jax.ShapeDtypeStruct((blocks, 7 * rows // blocks // 2, HD), jnp.bfloat16),
        in_specs=[pl.BlockSpec(memory_space=pltpu.SMEM), hbm, hbm, hbm, vmem],
        out_specs=vmem,
        scratch_shapes=[
            pltpu.VMEM(own.shape, own.dtype),
            pltpu.VMEM(own.shape, own.dtype),
            pltpu.SemaphoreType.DMA((4,)),
        ],
        compiler_params=pltpu.CompilerParams(vmem_limit_bytes=24 * 1024 * 1024),
        cost_estimate=cost(4 * rows * features * 4 * HD, 4 * own.size + 2 * gathered.size),
    )(core.reshape(1), in_hbm(own), in_hbm(far), in_hbm(near), gathered)


def turned(value, cosine, sine):
    return value * cosine + pltpu.roll(value, HALF, 1) * sine


def added(ref, parity, rows):
    value = ref[parity, rows].astype(jnp.float32)
    for j in range(parity + 2, ref.shape[0], 2):
        value = value + ref[j, rows].astype(jnp.float32)
    return value


def keys_and_values(part_ref, bias_ref, cos_ref, sin_ref, *rest):
    out_ref = rest[-1]
    size = out_ref.shape[1] // 2
    rows = slice(0, size)
    key = added(part_ref, 0, rows) + bias_ref[SHARE : SHARE + 1]
    key = turned(key, cos_ref[...], sin_ref[...]).astype(jnp.bfloat16)
    val = (added(part_ref, 1, rows) + bias_ref[SHARE + 1 : SHARE + 2]).astype(jnp.bfloat16)
    for j in range(out_ref.shape[0]):
        out_ref[j, :size] = key
        out_ref[j, size:] = val


def first_block(rank, blocks, window):
    return jnp.clip(rank - (window - 1), 0, blocks - window)


def queries(rank_ref, part_ref, bias_ref, cos_ref, sin_ref, seg_ref, mine_ref, out_ref, mask_ref):
    size = out_ref.shape[1]
    blocks = seg_ref.shape[0]
    window = mask_ref.shape[1] // size
    rank = rank_ref[0]
    first = first_block(rank, blocks, window)
    low = lanes_below_half((size // 2, HD))
    left = added(part_ref, 0, slice(3 * size, 7 * size // 2))
    right = added(part_ref, 1, slice(3 * size, 7 * size // 2))
    middle = jnp.concatenate(
        [
            jnp.where(low, left, pltpu.roll(right, HALF, 1)),
            jnp.where(low, pltpu.roll(left, HALF, 1), right),
        ],
        axis=0,
    )
    heads = [
        added(part_ref, 0, slice(size, 2 * size)),
        added(part_ref, 0, slice(2 * size, 3 * size)),
        middle,
        added(part_ref, 1, slice(size, 2 * size)),
        added(part_ref, 1, slice(2 * size, 3 * size)),
    ]
    cosine, sine = cos_ref[...], sin_ref[...]
    for h in range(SHARE):
        query = turned(heads[h] + bias_ref[h : h + 1], cosine, sine)
        out_ref[h] = query.astype(jnp.bfloat16)
    row = rank * size + lax.broadcasted_iota(jnp.int32, (size, size), 0)
    lane = lax.broadcasted_iota(jnp.int32, (size, size), 1)
    for b in range(window):
        seg = seg_ref[pl.ds(first + b, 1), :]
        allowed = (mine_ref[...] == seg) & ((first + b) * size + lane <= row)
        mask_ref[:, b * size : (b + 1) * size] = jnp.where(allowed, 0.0, -1e30)


def attend(rank_ref, q_ref, mask_ref, kv_ref, out_ref):
    size = out_ref.shape[0]
    blocks = kv_ref.shape[0]
    window = mask_ref.shape[1] // size
    first = first_block(rank_ref[0], blocks, window)
    span = kv_ref[pl.ds(first, window)]
    keys = span[:, :size].reshape(window * size, HD)
    vals = span[:, size:].reshape(window * size, HD)
    mask = mask_ref[...]
    for h in range(SHARE):
        scores = lax.dot_general(
            q_ref[h], keys, (((1,), (1,)), ((), ())), preferred_element_type=jnp.float32
        )
        scores = scores * (1.0 / HD**0.5) + mask
        top = jnp.max(scores, axis=-1, keepdims=True)
        expo = jnp.exp(scores - top)
        share = 1.0 / jnp.sum(expo, axis=-1, keepdims=True)
        weights = (expo * share).astype(jnp.bfloat16)
        context = jnp.dot(weights, vals, preferred_element_type=jnp.float32)
        out_ref[:, h * HD : (h + 1) * HD] = context.astype(jnp.bfloat16)


def body(tokens, ref_qkv, ref_bias, segment_ids, policy_key):
    replicas = lax.axis_size("rep")
    shards = lax.axis_size("fsdp")
    rows, features = tokens.shape
    mine = rows // replicas
    rank = lax.axis_index("rep")
    bf16, f32 = jnp.bfloat16, jnp.float32
    length = shards // SIDES
    shard = lax.axis_index("fsdp")

    def swapped(value, axis, bit):
        pairs = [(i, i ^ bit) for i in range(lax.axis_size(axis))]
        return lax.ppermute(value, axis, pairs)

    def passed(value, by):
        pairs = [(i, i // length * length + (i + by) % length) for i in range(shards)]
        return lax.ppermute(value, "fsdp", pairs)

    own_features, width = policy_key.shape
    keep, give = split_columns(rank, in_hbm(ref_qkv), in_hbm(policy_key))
    got = swapped(give, "rep", 1)
    core = lax.axis_index("tp") & 1
    fetched = lax.dynamic_slice_in_dim(tokens, core * (rows // 2), rows // 2, 0)
    far = swapped(fetched, "rep", 1)
    near = swapped(far, "tp", 1)
    copies = jax.ShapeDtypeStruct((shards, own_features, 7 * HD), bf16)
    pair = jax.ShapeDtypeStruct((2, own_features, width), bf16)
    copies, pair = call(pack, (copies, pair), 0, keep, got)
    column = pair
    for step in (1 << bit for bit in range(1, replicas.bit_length() - 1)):
        pairs = [((i - step if i % 2 else i + step) % replicas, i) for i in range(replicas)]
        column = jnp.concatenate([column, lax.ppermute(column, "rep", pairs)])
    gathered = exchanged(copies, "fsdp").reshape(features, -1)
    both = jnp.stack([column, swapped(column, "fsdp", length)])
    up, down = [both], [both]
    for k in range(1, length // 2 + 1):
        up.append(passed(up[-1], 1))
        if k < length // 2 or length == 1:
            down.append(passed(down[-1], -1))
    place = jnp.stack([shard % length, shard // length, rank]).astype(jnp.int32)
    whole = arranged(place, up + down[:0:-1]).reshape(-1, width)

    seg = segment_ids[0]
    start = rank * mine
    my_seg = lax.dynamic_slice_in_dim(seg, start, mine, 0)
    before = jnp.sum((seg[None, :] < my_seg[:, None]).astype(jnp.int32), axis=1)
    pos = start + jnp.arange(mine, dtype=jnp.int32) - before
    freq = 1000000.0 ** (-2.0 * jnp.arange(HALF, dtype=f32) / HD)
    angle = pos.astype(f32)[:, None] * freq[None, :]
    cosine, sine = jnp.cos(angle), jnp.sin(angle)
    cosine = jnp.concatenate([cosine, cosine], axis=1)
    sine = jnp.concatenate([-sine, sine], axis=1)
    bias = ref_bias.reshape(SHARE + 2, HD)

    part = projected(core, tokens, far, near, gathered, replicas)
    part = exchanged(part, "rep")
    my_kv = call(
        keys_and_values,
        (jax.ShapeDtypeStruct((replicas, 2 * mine, HD), bf16),),
        16 * mine * HD,
        part,
        bias,
        cosine,
        sine,
    )
    all_kv = exchanged(my_kv, "rep")
    window = min(WINDOW, replicas)
    query, mask = call(
        queries,
        (
            jax.ShapeDtypeStruct((SHARE, mine, HD), bf16),
            jax.ShapeDtypeStruct((mine, window * mine), f32),
        ),
        32 * SHARE * mine * HD,
        rank.reshape(1),
        part,
        bias,
        cosine,
        sine,
        seg.reshape(replicas, mine),
        my_seg[:, None],
        scalars=1,
    )
    context = call(
        attend,
        (jax.ShapeDtypeStruct((mine, SHARE * HD), bf16),),
        4 * SHARE * mine * window * mine * HD,
        rank.reshape(1),
        query,
        mask,
        all_kv,
        scalars=1,
    )
    return (context, whole)


def solution(mesh):
    in_specs = (
        P("fsdp", "rep"),
        P(("rep", "fsdp"), "tp"),
        P("tp"),
        P("fsdp", None),
        P(("rep", "fsdp"), "tp"),
    )
    out_specs = (P(("fsdp", "rep"), "tp"), P(None, "tp"))
    return jax.shard_map(body, mesh=mesh, in_specs=in_specs, out_specs=out_specs, check_vma=False)
```

```python
import jax
import jax.numpy as jnp
from jax import lax
from jax.experimental import pallas as pl
from jax.experimental.pallas import tpu as pltpu
from jax.sharding import PartitionSpec as P


QH = 40
KVH = 8
HD = 128
HALF = HD // 2
SHARE = QH // KVH
SIDES = 2
WINDOW = 5


def exchanged(blocks, axis):
    return lax.all_to_all(blocks, axis, split_axis=0, concat_axis=0, tiled=True)


def in_hbm(array):
    return pltpu.with_memory_space_constraint(array, pltpu.HBM)


def cost(flops, moved):
    return pl.CostEstimate(flops=flops, bytes_accessed=moved, transcendentals=0)


def call(kernel, outs, flops, *args, scalars=0):
    vmem = pl.BlockSpec(memory_space=pltpu.VMEM)
    smem = pl.BlockSpec(memory_space=pltpu.SMEM)
    moved = sum(a.size * a.dtype.itemsize for a in (*args, *outs))
    return pl.pallas_call(
        kernel,
        out_shape=outs if len(outs) > 1 else outs[0],
        in_specs=[smem] * scalars + [vmem] * (len(args) - scalars),
        out_specs=tuple(vmem for _ in outs) if len(outs) > 1 else vmem,
        compiler_params=pltpu.CompilerParams(vmem_limit_bytes=24 * 1024 * 1024),
        cost_estimate=cost(flops, moved),
    )(*args)


def lanes_below_half(shape):
    return lax.broadcasted_iota(jnp.int32, shape, len(shape) - 1) < HALF


def split(rank_ref, w_hbm, policy_hbm, keep_ref, give_ref, w_ref, policy_ref, sems):
    loads = [
        pltpu.make_async_copy(w_hbm, w_ref, sems.at[0]),
        pltpu.make_async_copy(policy_hbm, policy_ref, sems.at[1]),
    ]
    for load in loads:
        load.start()
    for load in loads:
        load.wait()
    key, val = w_ref[:, 5 * HD : 6 * HD], w_ref[:, 6 * HD :]
    low, high = w_ref[:, : 2 * HD], w_ref[:, 3 * HD : 5 * HD]
    left, right = w_ref[:, 2 * HD : 2 * HD + HALF], w_ref[:, 2 * HD + HALF : 3 * HD]
    odd = jnp.bitwise_and(rank_ref[0], 1)

    @pl.when(odd == 0)
    def _():
        keep_ref[...] = jnp.concatenate([key, low, left, policy_ref[...]], axis=1)
        give_ref[...] = jnp.concatenate([right, val, high, policy_ref[...]], axis=1)

    @pl.when(odd == 1)
    def _():
        keep_ref[...] = jnp.concatenate([val, high, right, policy_ref[...]], axis=1)
        give_ref[...] = jnp.concatenate([left, key, low, policy_ref[...]], axis=1)


def split_columns(rank, w, policy):
    vmem = pl.BlockSpec(memory_space=pltpu.VMEM)
    hbm = pl.BlockSpec(memory_space=pltpu.HBM)
    rows = w.shape[0]
    return pl.pallas_call(
        split,
        out_shape=(jax.ShapeDtypeStruct((rows, 7 * HALF + policy.shape[1]), w.dtype),) * 2,
        in_specs=[pl.BlockSpec(memory_space=pltpu.SMEM), hbm, hbm],
        out_specs=(vmem, vmem),
        scratch_shapes=[
            pltpu.VMEM(w.shape, w.dtype),
            pltpu.VMEM(policy.shape, policy.dtype),
            pltpu.SemaphoreType.DMA((2,)),
        ],
        compiler_params=pltpu.CompilerParams(vmem_limit_bytes=4 * 1024 * 1024),
        cost_estimate=cost(0, 8 * w.size),
    )(rank.reshape(1), w, policy)


def pack(keep_ref, got_ref, out_ref, pair_ref):
    row = jnp.concatenate([keep_ref[:, : 7 * HALF], got_ref[:, : 7 * HALF]], axis=1)
    for j in range(out_ref.shape[0]):
        out_ref[j] = row
    pair_ref[0] = keep_ref[:, 7 * HALF :]
    pair_ref[1] = got_ref[:, 7 * HALF :]


def arrange(place_ref, *refs):
    *parts, out_ref, sem = refs
    x, y, z = place_ref[0], place_ref[1], place_ref[2]
    length, sides, replicas = len(parts), out_ref.shape[1], out_ref.shape[0]
    copies = []
    for k, part in enumerate(parts):
        distance = k if k <= length // 2 else k - length
        column = jnp.bitwise_and(x - distance, length - 1)
        for side in range(sides):
            for b in range(replicas):
                place = out_ref.at[z ^ b, y ^ side, column]
                copies.append(pltpu.make_async_copy(part.at[side, b], place, sem))
    for copy in copies:
        copy.start()
    pltpu.make_async_copy(out_ref, out_ref, sem).wait()


def arranged(place, parts):
    sides, replicas, rows, width = parts[0].shape
    hbm = pl.BlockSpec(memory_space=pl.ANY)
    return pl.pallas_call(
        arrange,
        out_shape=jax.ShapeDtypeStruct((replicas, sides, len(parts), rows, width), parts[0].dtype),
        in_specs=[pl.BlockSpec(memory_space=pltpu.SMEM)] + [hbm] * len(parts),
        out_specs=hbm,
        scratch_shapes=[pltpu.SemaphoreType.DMA],
        compiler_params=pltpu.CompilerParams(vmem_limit_bytes=1024 * 1024),
        cost_estimate=cost(0, 4 * len(parts) * parts[0].size),
    )(place, *parts)


def project(core_ref, own_hbm, far_hbm, near_hbm, w_ref, out_ref, own_ref, other_ref, sems):
    blocks = out_ref.shape[0]
    rows = own_hbm.shape[0]
    step = rows // 2
    core = core_ref[0]
    loads = []
    for part in range(2):
        span = pl.ds(part * step, step)
        loads.append(pltpu.make_async_copy(own_hbm.at[span], own_ref.at[span], sems.at[part]))
    for source, index in ((far_hbm, core), (near_hbm, 1 - core)):
        span = pl.ds(pl.multiple_of(index * step, step), step)
        loads.append(pltpu.make_async_copy(source, other_ref.at[span], sems.at[len(loads)]))
    for load in loads:
        load.start()
    shared = w_ref[:, 3 * HD : 4 * HD]
    w_own = w_ref[:, : 4 * HD]
    swapped = pltpu.roll(shared.astype(jnp.float32), HALF, 1).astype(jnp.bfloat16)
    w_other = jnp.concatenate([w_ref[:, 4 * HD :], swapped], axis=1)
    size = rows // blocks
    low = lanes_below_half((size // 2, HD))
    for part in range(2):
        at = part * step
        loads[part].wait()
        if part == 0:
            loads[2].wait()
            loads[3].wait()
        value = jnp.dot(own_ref[at : at + step, :], w_own, preferred_element_type=jnp.float32)
        value = value + jnp.dot(
            other_ref[at : at + step, :], w_other, preferred_element_type=jnp.float32
        )
        for b in range(step // size):
            j = at // size + b
            piece = value[b * size : (b + 1) * size]
            for c in range(3):
                out_ref[j, c * size : (c + 1) * size] = piece[:, c * HD : (c + 1) * HD].astype(
                    jnp.bfloat16
                )
            last = piece[:, 3 * HD :]
            packed = jnp.where(low, last[: size // 2], pltpu.roll(last[size // 2 :], HALF, 1))
            out_ref[j, 3 * size :] = packed.astype(jnp.bfloat16)


def projected(core, own, far, near, gathered, blocks):
    rows, features = own.shape
    vmem = pl.BlockSpec(memory_space=pltpu.VMEM)
    hbm = pl.BlockSpec(memory_space=pltpu.HBM)
    return pl.pallas_call(
        project,
        out_shape=jax.ShapeDtypeStruct((blocks, 7 * rows // blocks // 2, HD), jnp.bfloat16),
        in_specs=[pl.BlockSpec(memory_space=pltpu.SMEM), hbm, hbm, hbm, vmem],
        out_specs=vmem,
        scratch_shapes=[
            pltpu.VMEM(own.shape, own.dtype),
            pltpu.VMEM(own.shape, own.dtype),
            pltpu.SemaphoreType.DMA((4,)),
        ],
        compiler_params=pltpu.CompilerParams(vmem_limit_bytes=24 * 1024 * 1024),
        cost_estimate=cost(4 * rows * features * 4 * HD, 4 * own.size + 2 * gathered.size),
    )(core.reshape(1), in_hbm(own), in_hbm(far), in_hbm(near), gathered)


def turned(value, cosine, sine):
    return value * cosine + pltpu.roll(value, HALF, 1) * sine


def added(ref, parity, rows):
    value = ref[parity, rows].astype(jnp.float32)
    for j in range(parity + 2, ref.shape[0], 2):
        value = value + ref[j, rows].astype(jnp.float32)
    return value


def keys_and_values(part_ref, bias_ref, cos_ref, sin_ref, *rest):
    out_ref = rest[-1]
    size = out_ref.shape[1] // 2
    rows = slice(0, size)
    key = added(part_ref, 0, rows) + bias_ref[SHARE : SHARE + 1]
    key = turned(key, cos_ref[...], sin_ref[...]).astype(jnp.bfloat16)
    val = (added(part_ref, 1, rows) + bias_ref[SHARE + 1 : SHARE + 2]).astype(jnp.bfloat16)
    for j in range(out_ref.shape[0]):
        out_ref[j, :size] = key
        out_ref[j, size:] = val


def first_block(rank, blocks, window):
    return jnp.clip(rank - (window - 1), 0, blocks - window)


def queries(rank_ref, part_ref, bias_ref, cos_ref, sin_ref, seg_ref, mine_ref, out_ref, mask_ref):
    size = out_ref.shape[1]
    blocks = seg_ref.shape[0]
    window = mask_ref.shape[1] // size
    rank = rank_ref[0]
    first = first_block(rank, blocks, window)
    low = lanes_below_half((size // 2, HD))
    left = added(part_ref, 0, slice(3 * size, 7 * size // 2))
    right = added(part_ref, 1, slice(3 * size, 7 * size // 2))
    middle = jnp.concatenate(
        [
            jnp.where(low, left, pltpu.roll(right, HALF, 1)),
            jnp.where(low, pltpu.roll(left, HALF, 1), right),
        ],
        axis=0,
    )
    heads = [
        added(part_ref, 0, slice(size, 2 * size)),
        added(part_ref, 0, slice(2 * size, 3 * size)),
        middle,
        added(part_ref, 1, slice(size, 2 * size)),
        added(part_ref, 1, slice(2 * size, 3 * size)),
    ]
    cosine, sine = cos_ref[...], sin_ref[...]
    for h in range(SHARE):
        query = turned(heads[h] + bias_ref[h : h + 1], cosine, sine)
        out_ref[h] = query.astype(jnp.bfloat16)
    row = rank * size + lax.broadcasted_iota(jnp.int32, (size, size), 0)
    lane = lax.broadcasted_iota(jnp.int32, (size, size), 1)
    for b in range(window):
        seg = seg_ref[pl.ds(first + b, 1), :]
        allowed = (mine_ref[...] == seg) & ((first + b) * size + lane <= row)
        mask_ref[:, b * size : (b + 1) * size] = jnp.where(allowed, 0.0, -1e30)


def attend(rank_ref, q_ref, mask_ref, kv_ref, out_ref):
    size = out_ref.shape[0]
    blocks = kv_ref.shape[0]
    window = mask_ref.shape[1] // size
    first = first_block(rank_ref[0], blocks, window)
    span = kv_ref[pl.ds(first, window)]
    keys = span[:, :size].reshape(window * size, HD)
    vals = span[:, size:].reshape(window * size, HD)
    mask = mask_ref[...]
    for h in range(SHARE):
        scores = lax.dot_general(
            q_ref[h], keys, (((1,), (1,)), ((), ())), preferred_element_type=jnp.float32
        )
        scores = scores * (1.0 / HD**0.5) + mask
        top = jnp.max(scores, axis=-1, keepdims=True)
        expo = jnp.exp(scores - top)
        share = 1.0 / jnp.sum(expo, axis=-1, keepdims=True)
        weights = (expo * share).astype(jnp.bfloat16)
        context = jnp.dot(weights, vals, preferred_element_type=jnp.float32)
        out_ref[:, h * HD : (h + 1) * HD] = context.astype(jnp.bfloat16)


def body(tokens, ref_qkv, ref_bias, segment_ids, policy_key):
    replicas = lax.axis_size("rep")
    shards = lax.axis_size("fsdp")
    rows, features = tokens.shape
    mine = rows // replicas
    rank = lax.axis_index("rep")
    bf16, f32 = jnp.bfloat16, jnp.float32
    length = shards // SIDES
    shard = lax.axis_index("fsdp")

    def swapped(value, axis, bit):
        pairs = [(i, i ^ bit) for i in range(lax.axis_size(axis))]
        return lax.ppermute(value, axis, pairs)

    def passed(value, by):
        pairs = [(i, i // length * length + (i + by) % length) for i in range(shards)]
        return lax.ppermute(value, "fsdp", pairs)

    own_features, width = policy_key.shape
    keep, give = split_columns(rank, in_hbm(ref_qkv), in_hbm(policy_key))
    got = swapped(give, "rep", 1)
    core = lax.axis_index("tp") & 1
    fetched = lax.dynamic_slice_in_dim(tokens, core * (rows // 2), rows // 2, 0)
    far = swapped(fetched, "rep", 1)
    near = swapped(far, "tp", 1)
    copies = jax.ShapeDtypeStruct((shards, own_features, 7 * HD), bf16)
    pair = jax.ShapeDtypeStruct((2, own_features, width), bf16)
    copies, pair = call(pack, (copies, pair), 0, keep, got)
    pairs = [pair] + [swapped(pair, "rep", bit) for bit in range(2, replicas, 2)]
    column = jnp.concatenate(pairs)
    gathered = exchanged(copies, "fsdp").reshape(features, -1)
    both = jnp.stack([column, swapped(column, "fsdp", length)])
    up, down = [both], [both]
    for k in range(1, length // 2 + 1):
        up.append(passed(up[-1], 1))
        if k < length // 2 or length == 1:
            down.append(passed(down[-1], -1))
    place = jnp.stack([shard % length, shard // length, rank]).astype(jnp.int32)
    whole = arranged(place, up + down[:0:-1]).reshape(-1, width)

    seg = segment_ids[0]
    start = rank * mine
    my_seg = lax.dynamic_slice_in_dim(seg, start, mine, 0)
    before = jnp.sum((seg[None, :] < my_seg[:, None]).astype(jnp.int32), axis=1)
    pos = start + jnp.arange(mine, dtype=jnp.int32) - before
    freq = 1000000.0 ** (-2.0 * jnp.arange(HALF, dtype=f32) / HD)
    angle = pos.astype(f32)[:, None] * freq[None, :]
    cosine, sine = jnp.cos(angle), jnp.sin(angle)
    cosine = jnp.concatenate([cosine, cosine], axis=1)
    sine = jnp.concatenate([-sine, sine], axis=1)
    bias = ref_bias.reshape(SHARE + 2, HD)

    part = projected(core, tokens, far, near, gathered, replicas)
    part = exchanged(part, "rep")
    my_kv = call(
        keys_and_values,
        (jax.ShapeDtypeStruct((replicas, 2 * mine, HD), bf16),),
        16 * mine * HD,
        part,
        bias,
        cosine,
        sine,
    )
    all_kv = exchanged(my_kv, "rep")
    window = min(WINDOW, replicas)
    query, mask = call(
        queries,
        (
            jax.ShapeDtypeStruct((SHARE, mine, HD), bf16),
            jax.ShapeDtypeStruct((mine, window * mine), f32),
        ),
        32 * SHARE * mine * HD,
        rank.reshape(1),
        part,
        bias,
        cosine,
        sine,
        seg.reshape(replicas, mine),
        my_seg[:, None],
        scalars=1,
    )
    context = call(
        attend,
        (jax.ShapeDtypeStruct((mine, SHARE * HD), bf16),),
        4 * SHARE * mine * window * mine * HD,
        rank.reshape(1),
        query,
        mask,
        all_kv,
        scalars=1,
    )
    return (context, whole)


def solution(mesh):
    in_specs = (
        P("fsdp", "rep"),
        P(("rep", "fsdp"), "tp"),
        P("tp"),
        P("fsdp", None),
        P(("rep", "fsdp"), "tp"),
    )
    out_specs = (P(("fsdp", "rep"), "tp"), P(None, "tp"))
    return jax.shard_map(body, mesh=mesh, in_specs=in_specs, out_specs=out_specs, check_vma=False)
```
